32 devices in a mesh: dp: 2 (over z, core), tp: 16 (over x, y).
Axes of the slice: x: 4, y: 4, z: 1, core: 2. Of those that a mesh axis runs over, the one named last changes fastest.
The devices are a block of a 4x4x8 slice.
Arguments:
- x: bfloat16 [4096, 2048], P('dp'), parts along dimension 0
- w_gate: bfloat16 [2048, 16384], P(None, 'tp')
- w_up: bfloat16 [2048, 16384], P(None, 'tp')
- w_down: bfloat16 [16384, 2048], P('tp')
Outputs:
- output: bfloat16 [4096, 2048], P('dp'), parts along dimension 0
There are 2 independent parts. The reference program is written for one: setup_inputs(seed, part) draws one part's arguments, and reference() takes and returns one part's arrays. A program takes and returns all parts, laid end to end along the dimension named above; an argument that names none is the same for every part.
All inputs are finite; a program needn't handle non-finite values.
Results may differ from the reference program's by a relative error of at most 0.016.
Values are sent between devices in bfloat16 or wider.
A program may use at most 768 MiB of HBM per device.

```python
import jax
import jax.numpy as jnp

ROWS = 2048
D = 2048
FF = 16384


def setup_inputs(seed: int = 0, part: int = 0) -> dict:
    kx, kg, ku, kd = jax.random.split(jax.random.key(seed), 4)
    drawn = {
        "x": jax.random.normal(jax.random.fold_in(kx, part), (ROWS, D), jnp.float32),
        "w_gate": jax.random.normal(kg, (D, FF), jnp.float32) * D**-0.5,
        "w_up": jax.random.normal(ku, (D, FF), jnp.float32) * D**-0.5,
        "w_down": jax.random.normal(kd, (FF, D), jnp.float32) * FF**-0.5,
    }
    return {k: v.astype(jnp.bfloat16) for k, v in drawn.items()}


def reference(x, w_gate, w_up, w_down):
    gate = jnp.dot(x, w_gate, preferred_element_type=jnp.float32)
    up = jnp.dot(x, w_up, preferred_element_type=jnp.float32)
    hidden = (jax.nn.gelu(gate) * up).astype(jnp.bfloat16)
    return jnp.dot(hidden, w_down, preferred_element_type=jnp.float32).astype(jnp.bfloat16)
```

```python
import functools
import math

import jax
import jax.numpy as jnp
from jax import lax
from jax.experimental import pallas as pl
from jax.experimental.pallas import tpu as pltpu
from jax.sharding import PartitionSpec as P

MESH = pl.DeviceIdType.MESH
BLOCK = 256
HID = 256
OUT = 512


def kernel(side, x_hbm, wg_hbm, wu_hbm, wd_hbm, y, xb, wg, wu, wd, hid, term, own,
           s1s, s1r, s2s, s2r, s3s, s3r, s4s, s4r, x_sem, wg_sem, wu_sem, wd_sem,
           send_sem, recv_sem):
    rows, d = x_hbm.shape
    f = wg.shape[1]
    blocks = rows // BLOCK
    sec = BLOCK // side
    piece = sec // side
    half = d // 2
    quarter = half // 2
    slots = term.shape[0]
    f32, bf16 = jnp.float32, jnp.bfloat16

    me = lax.axis_index("tp")
    i, j = me // side, me % side

    def up1(v):
        return lax.rem(v + 1, side)

    def dn1(v):
        return lax.rem(v + side - 1, side)

    along_x = (up1(i) * side + j, dn1(i) * side + j)
    along_y = (i * side + up1(j), i * side + dn1(j))
    first = (along_x, along_y)
    second = (along_y, along_x)
    pos = ((i, j), (j, i))

    barrier = pltpu.get_barrier_semaphore()
    for n in along_x + along_y:
        pl.semaphore_signal(barrier, inc=1, device_id={"tp": n}, device_id_type=MESH)

    def x_copy(b):
        return pltpu.make_async_copy(
            x_hbm.at[pl.ds(pl.multiple_of(b * BLOCK, BLOCK), BLOCK)],
            xb.at[lax.rem(b, 2)], x_sem.at[lax.rem(b, 2)])

    def g_copy(n):
        return pltpu.make_async_copy(
            wg_hbm.at[:, pl.ds(n * HID, HID)], wg.at[:, pl.ds(n * HID, HID)], wg_sem.at[n])

    def u_copy(n):
        return pltpu.make_async_copy(
            wu_hbm.at[:, pl.ds(n * HID, HID)], wu.at[:, pl.ds(n * HID, HID)], wu_sem.at[n])

    def d_copy(n):
        return pltpu.make_async_copy(
            wd_hbm.at[:, pl.ds(n * OUT, OUT)], wd.at[:, pl.ds(n * OUT, OUT)], wd_sem.at[n])

    x_copy(0).start()
    for n in range(f // HID):
        g_copy(n).start()
        u_copy(n).start()
    for n in range(d // OUT):
        d_copy(n).start()

    def remote(src, dst, stage, b, t, way, to):
        return pltpu.make_async_remote_copy(
            src_ref=src, dst_ref=dst, send_sem=send_sem.at[stage, b, t, way],
            recv_sem=recv_sem.at[stage, b, t, way], device_id={"tp": to}, device_id_type=MESH)

    def ds(start, size):
        return pl.ds(pl.multiple_of(start, size), size)

    def compute(b):
        slot = lax.rem(b, slots)
        xs = lax.rem(b, 2)
        x_copy(b).wait()

        @pl.when(b + 1 < blocks)
        def _():
            x_copy(b + 1).start()

        for n in range(f // HID):
            cols = pl.ds(n * HID, HID)

            @pl.when(b == 0)
            def _():
                g_copy(n).wait()
                u_copy(n).wait()

            gate = jnp.dot(xb[xs], wg[:, cols], preferred_element_type=f32)
            up = jnp.dot(xb[xs], wu[:, cols], preferred_element_type=f32)
            hid[:, cols] = (jax.nn.gelu(gate) * up).astype(bf16)
        for n in range(d // OUT):
            cols = pl.ds(n * OUT, OUT)

            @pl.when(b == 0)
            def _():
                d_copy(n).wait()

            term[slot, :, cols] = jnp.dot(hid[...], wd[:, cols], preferred_element_type=f32)

    def copies(stage, b, t):
        p, q = pos[t]
        cols = pl.ds(t * half, half)
        lo, hi = pl.ds(t * half, quarter), pl.ds(t * half + quarter, quarter)
        base = b * BLOCK
        if stage == 0:
            up, dn = first[t]
            h = sec // 2
            return (remote(s1s.at[b, t, pl.ds(0, h)], s1r.at[b, t, 0], 0, b, t, 0, up),
                    remote(s1s.at[b, t, pl.ds(h, h)], s1r.at[b, t, 1], 0, b, t, 1, dn))
        if stage == 1:
            up, dn = first[t]
            return (remote(s2s.at[b, t, 0], s2r.at[b, t, 0], 1, b, t, 0, up),
                    remote(s2s.at[b, t, 1], s2r.at[b, t, 1], 1, b, t, 1, dn))
        if stage == 2:
            up, dn = second[t]
            return (remote(s3s.at[b, t, :, pl.ds(0, quarter)], s3r.at[b, t, 0], 2, b, t, 0, up),
                    remote(s3s.at[b, t, :, pl.ds(quarter, quarter)], s3r.at[b, t, 1], 2, b, t, 1, dn))
        if stage == 3:
            up, dn = second[t]
            return (remote(s4s.at[b, t, 0], s4r.at[b, t, 0], 3, b, t, 0, up),
                    remote(s4s.at[b, t, 1], s4r.at[b, t, 1], 3, b, t, 1, dn))
        if stage == 4:
            up, dn = second[t]
            at = y.at[ds(base + p * sec + q * piece, piece), cols]
            return remote(at, at, 4, b, t, 0, up), remote(at, at, 4, b, t, 1, dn)
        if stage == 5:
            up, dn = second[t]
            a0 = y.at[ds(base + p * sec + dn1(q) * piece, piece), lo]
            a1 = y.at[ds(base + p * sec + up1(q) * piece, piece), hi]
            return remote(a0, a0, 5, b, t, 0, up), remote(a1, a1, 5, b, t, 1, dn)
        if stage == 6:
            up, dn = first[t]
            at = y.at[ds(base + p * sec, sec), cols]
            return remote(at, at, 6, b, t, 0, up), remote(at, at, 6, b, t, 1, dn)
        up, dn = first[t]
        h = sec // 2
        a0 = y.at[ds(base + dn1(p) * sec, h), cols]
        a1 = y.at[ds(base + up1(p) * sec + h, h), cols]
        return remote(a0, a0, 7, b, t, 0, up), remote(a1, a1, 7, b, t, 1, dn)

    def arrivals(stage, b, t):
        p, q = pos[t]
        cols = pl.ds(t * half, half)
        lo, hi = pl.ds(t * half, quarter), pl.ds(t * half + quarter, quarter)
        base = b * BLOCK
        opp = lambda v: lax.rem(v + 2, side)
        if stage < 4:
            r = (s1r, s2r, s3r, s4r)[stage]
            at = (r.at[b, t, 0], r.at[b, t, 1])
        elif stage == 4:
            at = (y.at[ds(base + p * sec + dn1(q) * piece, piece), cols],
                  y.at[ds(base + p * sec + up1(q) * piece, piece), cols])
        elif stage == 5:
            row = ds(base + p * sec + opp(q) * piece, piece)
            at = (y.at[row, lo], y.at[row, hi])
        elif stage == 6:
            at = (y.at[ds(base + dn1(p) * sec, sec), cols],
                  y.at[ds(base + up1(p) * sec, sec), cols])
        else:
            h = sec // 2
            at = (y.at[ds(base + opp(p) * sec, h), cols],
                  y.at[ds(base + opp(p) * sec + h, h), cols])
        return tuple(remote(a, a, stage, b, t, way, me) for way, a in enumerate(at))

    def start(stage, b, t):
        for c in copies(stage, b, t):
            c.start()

    def arrive(stage, b, t):
        for c in arrivals(stage, b, t):
            c.wait_recv()

    def stage0(b):
        slot = lax.rem(b, slots)
        for t in range(2):
            p, _ = pos[t]
            rows_ = ds(lax.rem(p + 2, side) * sec, sec)
            s1s[b, t] = term[slot, rows_, pl.ds(t * half, half)].astype(bf16)
            start(0, b, t)

    def stage1(b):
        slot = lax.rem(b, slots)
        h = sec // 2
        for t in range(2):
            p, _ = pos[t]
            cols = pl.ds(t * half, half)
            arrive(0, b, t)
            r, l = up1(p) * sec, dn1(p) * sec
            s2s[b, t, 0, pl.ds(0, h)] = (
                term[slot, ds(r, h), cols] + s1r[b, t, 0].astype(f32)).astype(bf16)
            s2s[b, t, 0, pl.ds(h, h)] = term[slot, ds(r + h, h), cols].astype(bf16)
            s2s[b, t, 1, pl.ds(0, h)] = term[slot, ds(l, h), cols].astype(bf16)
            s2s[b, t, 1, pl.ds(h, h)] = (
                term[slot, ds(l + h, h), cols] + s1r[b, t, 1].astype(f32)).astype(bf16)
            start(1, b, t)

    def stage2(b):
        slot = lax.rem(b, slots)
        for t in range(2):
            p, q = pos[t]
            cols = pl.ds(t * half, half)
            arrive(1, b, t)
            own[b, t] = (term[slot, ds(p * sec, sec), cols]
                         + s2r[b, t, 0].astype(f32) + s2r[b, t, 1].astype(f32))
            s3s[b, t] = own[b, t, ds(lax.rem(q + 2, side) * piece, piece), :].astype(bf16)
            start(2, b, t)

    def stage3(b):
        lo, hi = pl.ds(0, quarter), pl.ds(quarter, quarter)
        for t in range(2):
            _, q = pos[t]
            arrive(2, b, t)
            r, l = ds(up1(q) * piece, piece), ds(dn1(q) * piece, piece)
            s4s[b, t, 0, :, lo] = (own[b, t, r, lo] + s3r[b, t, 0].astype(f32)).astype(bf16)
            s4s[b, t, 0, :, hi] = own[b, t, r, hi].astype(bf16)
            s4s[b, t, 1, :, lo] = own[b, t, l, lo].astype(bf16)
            s4s[b, t, 1, :, hi] = (own[b, t, l, hi] + s3r[b, t, 1].astype(f32)).astype(bf16)
            start(3, b, t)

    def stage4(b):
        for t in range(2):
            p, q = pos[t]
            arrive(3, b, t)
            y[ds(b * BLOCK + p * sec + q * piece, piece), pl.ds(t * half, half)] = (
                own[b, t, ds(q * piece, piece), :]
                + s4r[b, t, 0].astype(f32) + s4r[b, t, 1].astype(f32)).astype(bf16)
            start(4, b, t)

    def pass_on(stage):
        def run(b):
            for t in range(2):
                arrive(stage - 1, b, t)
                start(stage, b, t)
        return run

    def finish(b):
        for t in range(2):
            arrive(7, b, t)

    stages = [stage0, stage1, stage2, stage3, stage4, pass_on(5), pass_on(6), pass_on(7), finish]

    def step(n, _):
        @pl.when(n < blocks)
        def _():
            compute(n)

        @pl.when(n == 0)
        def _():
            pl.semaphore_wait(barrier, 4)

        for k, stage in enumerate(stages):
            @pl.when((n >= k) & (n < blocks + k))
            def _():
                stage(n - k)
        return 0

    lax.fori_loop(0, blocks + len(stages) - 1, step, 0)

    def drain(b, _):
        for stage in range(8):
            for t in range(2):
                for c in copies(stage, b, t):
                    c.wait_send()
        return 0

    lax.fori_loop(0, blocks, drain, 0)


def solution(mesh):
    side = math.isqrt(mesh.shape["tp"])

    def step(x, w_gate, w_up, w_down):
        rows, d = x.shape
        f = w_gate.shape[1]
        blocks, sec = rows // BLOCK, BLOCK // side
        piece, half = sec // side, d // 2
        bf16, f32 = jnp.bfloat16, jnp.float32
        return pl.pallas_call(
            functools.partial(kernel, side),
            out_shape=jax.ShapeDtypeStruct((rows, d), bf16),
            in_specs=[pl.BlockSpec(memory_space=pl.ANY)] * 4,
            out_specs=pl.BlockSpec(memory_space=pltpu.VMEM),
            scratch_shapes=[
                pltpu.VMEM((2, BLOCK, d), bf16),
                pltpu.VMEM((d, f), bf16),
                pltpu.VMEM((d, f), bf16),
                pltpu.VMEM((f, d), bf16),
                pltpu.VMEM((BLOCK, f), bf16),
                pltpu.VMEM((3, BLOCK, d), f32),
                pltpu.VMEM((blocks, 2, sec, half), f32),
                pltpu.VMEM((blocks, 2, sec, half), bf16),
                pltpu.VMEM((blocks, 2, 2, sec // 2, half), bf16),
                pltpu.VMEM((blocks, 2, 2, sec, half), bf16),
                pltpu.VMEM((blocks, 2, 2, sec, half), bf16),
                pltpu.VMEM((blocks, 2, piece, half), bf16),
                pltpu.VMEM((blocks, 2, 2, piece, half // 2), bf16),
                pltpu.VMEM((blocks, 2, 2, piece, half), bf16),
                pltpu.VMEM((blocks, 2, 2, piece, half), bf16),
                pltpu.SemaphoreType.DMA((2,)),
                pltpu.SemaphoreType.DMA((f // HID,)),
                pltpu.SemaphoreType.DMA((f // HID,)),
                pltpu.SemaphoreType.DMA((d // OUT,)),
                pltpu.SemaphoreType.DMA((8, blocks, 2, 2)),
                pltpu.SemaphoreType.DMA((8, blocks, 2, 2)),
            ],
            compiler_params=pltpu.CompilerParams(
                collective_id=0, has_side_effects=True, vmem_limit_bytes=60 * 2**20),
        )(x, w_gate, w_up, w_down)

    return jax.shard_map(
        step,
        mesh=mesh,
        in_specs=(P("dp", None), P(None, "tp"), P(None, "tp"), P("tp", None)),
        out_specs=P("dp", None),
        check_vma=False,
    )
```

```python
import functools
import math

import jax
import jax.numpy as jnp
from jax import lax
from jax.experimental import pallas as pl
from jax.experimental.pallas import tpu as pltpu
from jax.sharding import PartitionSpec as P

MESH = pl.DeviceIdType.MESH
BLOCK = 256
HID0, OUT0 = 256, 512
HID, OUT = 512, 1024
SPLIT = 5


def kernel(side, x_hbm, wg_hbm, wu_hbm, wd_hbm, y, xb, wg, wu, wd, hid, term, own,
           s1s, s1r, s2s, s2r, s3s, s3r, s4s, s4r, x_sem, wg_sem, wu_sem, wd_sem,
           send_sem, recv_sem):
    rows, d = x_hbm.shape
    f = wg.shape[1]
    blocks = rows // BLOCK
    pairs = blocks // 2
    sec = BLOCK // side
    piece = sec // side
    h = sec // 2
    half = d // 2
    quarter = half // 2
    slots = term.shape[0]
    f32, bf16 = jnp.float32, jnp.bfloat16

    me = lax.axis_index("tp")
    i, j = me // side, me % side

    def up1(v):
        return lax.rem(v + 1, side)

    def dn1(v):
        return lax.rem(v + side - 1, side)

    def opp(v):
        return lax.rem(v + 2, side)

    along_x = (up1(i) * side + j, dn1(i) * side + j)
    along_y = (i * side + up1(j), i * side + dn1(j))
    first = (along_x, along_y)
    second = (along_y, along_x)
    pos = ((i, j), (j, i))

    barrier = pltpu.get_barrier_semaphore()
    for n in along_x + along_y:
        pl.semaphore_signal(barrier, inc=1, device_id={"tp": n}, device_id_type=MESH)

    def ds(start, size):
        return pl.ds(pl.multiple_of(start, size), size)

    def x_copy(b):
        return pltpu.make_async_copy(
            x_hbm.at[ds(b * BLOCK, BLOCK)], xb.at[lax.rem(b, 2)], x_sem.at[lax.rem(b, 2)])

    pieces0 = [(0, HID0), (HID0, HID0), (2 * HID0, f - 2 * HID0)]

    def load(src, dst, sem, n, first_col, size):
        cols = pl.ds(first_col, size)
        return pltpu.make_async_copy(src.at[:, cols], dst.at[:, cols], sem.at[n])

    def load_in(n):
        return load(wg_hbm, wg, wg_sem, n, *pieces0[n]), load(wu_hbm, wu, wu_sem, n, *pieces0[n])

    def load_out(n):
        return load(wd_hbm, wd, wd_sem, n, n * OUT0, OUT0)

    x_copy(0).start()
    for n in range(3):
        for c in load_in(n):
            c.start()

    def hidden(xs, first_col, size):
        cols = pl.ds(first_col, size)
        gate = jnp.dot(xb[xs], wg[:, cols], preferred_element_type=f32)
        up = jnp.dot(xb[xs], wu[:, cols], preferred_element_type=f32)
        hid[:, cols] = (jax.nn.gelu(gate) * up).astype(bf16)

    def down(slot, n, size):
        cols = pl.ds(n * size, size)
        term[slot, :, cols] = jnp.dot(hid[...], wd[:, cols], preferred_element_type=f32)

    def compute1(b):
        x_copy(b).wait()
        for n in range(f // HID):
            hidden(lax.rem(b, 2), n * HID, HID)

    def compute2(b):
        for n in range(d // OUT):
            down(lax.rem(b, slots), n, OUT)

        @pl.when(b + 2 < blocks)
        def _():
            x_copy(b + 2).start()

    def compute(b):
        compute1(b)
        compute2(b)

    def cols_of(t):
        return pl.ds(t * half, half)

    def two(g):
        return pl.ds(2 * g, 2)

    def far(b, t):
        return [(s1s.at[t, b, pl.ds(w * h, h)], s1r.at[t, w, b], first[t][w]) for w in range(2)]

    def near(b, t):
        return [(s2s.at[t, w, b], s2r.at[t, w, b], first[t][w]) for w in range(2)]

    def near_part(b, t, own_half):
        k = [pl.ds((1 - w if own_half else w) * h, h) for w in range(2)]
        return [(s2s.at[t, w, b, k[w]], s2r.at[t, w, b, k[w]], first[t][w]) for w in range(2)]

    def far2(g, t):
        return [(s3s.at[t, two(g), :, pl.ds(w * quarter, quarter)], s3r.at[t, w, two(g)],
                 second[t][w]) for w in range(2)]

    def near2(g, t):
        return [(s4s.at[t, w, two(g)], s4r.at[t, w, two(g)], second[t][w]) for w in range(2)]

    def gather1(g, t):
        p, q = pos[t]
        at = y.at[two(g), ds(p * sec + q * piece, piece), cols_of(t)]
        return [(at, at, second[t][w]) for w in range(2)]

    def gather2(g, t):
        p, q = pos[t]
        at = [y.at[two(g), ds(p * sec + v * piece, piece), pl.ds(t * half + w * quarter, quarter)]
              for w, v in enumerate((dn1(q), up1(q)))]
        return [(at[w], at[w], second[t][w]) for w in range(2)]

    def gather3(bs, t):
        p, _ = pos[t]
        at = y.at[bs, ds(p * sec, sec), cols_of(t)]
        return [(at, at, first[t][w]) for w in range(2)]

    def gather4(bs, t):
        p, _ = pos[t]
        at = [y.at[bs, ds(v * sec + w * h, h), cols_of(t)] for w, v in enumerate((dn1(p), up1(p)))]
        return [(at[w], at[w], first[t][w]) for w in range(2)]

    FAR, NEAR, FAR2, NEAR2, G1, G2, G3, G4 = range(8)
    own_sem = 8 * blocks

    def start(copies, kind, sem):
        for src, dst, to in copies:
            pltpu.make_async_remote_copy(
                src_ref=src, dst_ref=dst, send_sem=send_sem.at[kind], recv_sem=recv_sem.at[sem],
                device_id={"tp": to}, device_id_type=MESH).start()

    def arrive(like, sem):
        pltpu.make_async_copy(like, like, recv_sem.at[sem]).wait()

    def base_of(kind):
        return kind * blocks

    def pack(b, t, split):
        slot = lax.rem(b, slots)
        p, _ = pos[t]
        c = cols_of(t)
        s1s[t, b] = term[slot, ds(opp(p) * sec, sec), c].astype(bf16)
        start(far(b, t), FAR, base_of(FAR) + b)
        s2s[t, 0, b, pl.ds(h, h)] = term[slot, ds(up1(p) * sec + h, h), c].astype(bf16)
        s2s[t, 1, b, pl.ds(0, h)] = term[slot, ds(dn1(p) * sec, h), c].astype(bf16)
        if split:
            start(near_part(b, t, True), NEAR, own_sem + b)

    def reduce1(b, split):
        slot = lax.rem(b, slots)
        arrive(s1r.at[:, :, b], base_of(FAR) + b)
        for t in range(2):
            p, _ = pos[t]
            c = cols_of(t)
            s2s[t, 0, b, pl.ds(0, h)] = (
                term[slot, ds(up1(p) * sec, h), c] + s1r[t, 0, b].astype(f32)).astype(bf16)
            s2s[t, 1, b, pl.ds(h, h)] = (
                term[slot, ds(dn1(p) * sec + h, h), c] + s1r[t, 1, b].astype(f32)).astype(bf16)
            start(near_part(b, t, False) if split else near(b, t), NEAR, base_of(NEAR) + b)

    def reduce2(g):
        for b in (2 * g, 2 * g + 1):
            if b < SPLIT:
                arrive(s1r.at[:, :, b], own_sem + b)
                arrive(s1r.at[:, :, b], base_of(NEAR) + b)
            else:
                arrive(s2r.at[:, :, b], base_of(NEAR) + b)
        for t in range(2):
            p, q = pos[t]
            for b in (2 * g, 2 * g + 1):
                own[t, b] = (term[b % slots, ds(p * sec, sec), cols_of(t)]
                             + s2r[t, 0, b].astype(f32) + s2r[t, 1, b].astype(f32))
                s3s[t, b] = own[t, b, ds(opp(q) * piece, piece), :].astype(bf16)
            start(far2(g, t), FAR2, base_of(FAR2) + g)

    def reduce3(g):
        lo, hi = pl.ds(0, quarter), pl.ds(quarter, quarter)
        arrive(s3r.at[:, :, two(g)], base_of(FAR2) + g)
        for t in range(2):
            _, q = pos[t]
            r, l = ds(up1(q) * piece, piece), ds(dn1(q) * piece, piece)
            for b in (2 * g, 2 * g + 1):
                s4s[t, 0, b, :, lo] = (own[t, b, r, lo] + s3r[t, 0, b].astype(f32)).astype(bf16)
                s4s[t, 0, b, :, hi] = own[t, b, r, hi].astype(bf16)
                s4s[t, 1, b, :, lo] = own[t, b, l, lo].astype(bf16)
                s4s[t, 1, b, :, hi] = (own[t, b, l, hi] + s3r[t, 1, b].astype(f32)).astype(bf16)
            start(near2(g, t), NEAR2, base_of(NEAR2) + g)

    def reduce4(g):
        arrive(s4r.at[:, :, two(g)], base_of(NEAR2) + g)
        for t in range(2):
            p, q = pos[t]
            for b in (2 * g, 2 * g + 1):
                y[b, ds(p * sec + q * piece, piece), cols_of(t)] = (
                    own[t, b, ds(q * piece, piece), :]
                    + s4r[t, 0, b].astype(f32) + s4r[t, 1, b].astype(f32)).astype(bf16)
            start(gather1(g, t), G1, base_of(G1) + g)

    def send2(g):
        arrive(s4r.at[:, :, two(g)], base_of(G1) + g)
        for t in range(2):
            start(gather2(g, t), G2, base_of(G2) + g)

    def units(g):
        return [(two(g), g)] if g < pairs - 1 else [(pl.ds(b, 1), b) for b in (2 * g, 2 * g + 1)]

    def send3(g):
        arrive(s3r.at[:, :, two(g)], base_of(G2) + g)
        for bs, u in units(g):
            for t in range(2):
                start(gather3(bs, t), G3, base_of(G3) + u)

    def send4(g, n=None):
        for k, (bs, u) in enumerate(units(g)):
            if n is None or n == k:
                arrive(s2r.at[:, :, bs], base_of(G3) + u)
                for t in range(2):
                    start(gather4(bs, t), G4, base_of(G4) + u)

    x_copy(0).wait()
    for n in range(3):
        for c in load_in(n):
            c.wait()
        if n == 1:
            for k in range(d // OUT0):
                load_out(k).start()
            x_copy(1).start()
        hidden(0, *pieces0[n])
    for t in range(2):
        for n in range(t * half // OUT0, (t + 1) * half // OUT0):
            load_out(n).wait()
            down(0, n, OUT0)
        if t == 0:
            pl.semaphore_wait(barrier, 4)
        pack(0, t, True)
    x_copy(2).start()

    compute1(1)
    reduce1(0, True)
    compute2(1)
    pack(1, 0, True)
    pack(1, 1, True)

    beside = {
        3: [(reduce2, 0)],
        4: [(reduce3, 0)],
        5: [(reduce2, 1), (reduce4, 0)],
        6: [(reduce3, 1), (send2, 0)],
        7: [(reduce2, 2), (reduce4, 1), (send3, 0)],
    }

    def step(b, _):
        compute(b)

        @pl.when(b < SPLIT)
        def _():
            pack(b, 0, True)
            pack(b, 1, True)

        @pl.when(b >= SPLIT)
        def _():
            pack(b, 0, False)
            pack(b, 1, False)

        @pl.when(b <= SPLIT)
        def _():
            reduce1(b - 1, True)

        @pl.when(b > SPLIT)
        def _():
            reduce1(b - 1, False)

        for k, tasks in beside.items():
            @pl.when(b == k)
            def _():
                for task, g in tasks:
                    task(g)
        return 0

    lax.fori_loop(2, blocks, step, 0)

    reduce1(blocks - 1, SPLIT == blocks)
    for task, *args in [
        (reduce3, 2), (send2, 1),
        (reduce2, 3), (reduce4, 2), (send3, 1),
        (reduce3, 3), (send2, 2), (send4, 0),
        (reduce4, 3), (send3, 2),
        (send2, 3), (send4, 1),
        (send3, 3), (send4, 2), (send4, 3, 0), (send4, 3, 1),
    ]:
        task(*args)
    for g in range(pairs):
        for bs, u in units(g):
            arrive(s1r.at[:, :, bs], base_of(G4) + u)

    for kind, like in enumerate((s1s, s2s, s3s, s4s, s4s, s3s, s2s, s1s)):
        pltpu.make_async_copy(like, like, send_sem.at[kind]).wait()


def solution(mesh):
    side = math.isqrt(mesh.shape["tp"])

    def step(x, w_gate, w_up, w_down):
        rows, d = x.shape
        f = w_gate.shape[1]
        blocks, sec = rows // BLOCK, BLOCK // side
        piece, half = sec // side, d // 2
        bf16, f32 = jnp.bfloat16, jnp.float32
        return pl.pallas_call(
            functools.partial(kernel, side),
            out_shape=pltpu.VMEM((blocks, BLOCK, d), bf16),
            in_specs=[pl.BlockSpec(memory_space=pl.ANY)] * 4,
            out_specs=pl.BlockSpec(memory_space=pltpu.VMEM),
            scratch_shapes=[
                pltpu.VMEM((2, BLOCK, d), bf16),
                pltpu.VMEM((d, f), bf16),
                pltpu.VMEM((d, f), bf16),
                pltpu.VMEM((f, d), bf16),
                pltpu.VMEM((BLOCK, f), bf16),
                pltpu.VMEM((4, BLOCK, d), f32),
                pltpu.VMEM((2, blocks, sec, half), f32),
                pltpu.VMEM((2, blocks, sec, half), bf16),
                pltpu.VMEM((2, 2, blocks, sec // 2, half), bf16),
                pltpu.VMEM((2, 2, blocks, sec, half), bf16),
                pltpu.VMEM((2, 2, blocks, sec, half), bf16),
                pltpu.VMEM((2, blocks, piece, half), bf16),
                pltpu.VMEM((2, 2, blocks, piece, half // 2), bf16),
                pltpu.VMEM((2, 2, blocks, piece, half), bf16),
                pltpu.VMEM((2, 2, blocks, piece, half), bf16),
                pltpu.SemaphoreType.DMA((2,)),
                pltpu.SemaphoreType.DMA((3,)),
                pltpu.SemaphoreType.DMA((3,)),
                pltpu.SemaphoreType.DMA((d // OUT0,)),
                pltpu.SemaphoreType.DMA((8,)),
                pltpu.SemaphoreType.DMA((8 * blocks + SPLIT,)),
            ],
            compiler_params=pltpu.CompilerParams(
                collective_id=0, has_side_effects=True, vmem_limit_bytes=50 * 2**20),
        )(x, w_gate, w_up, w_down).reshape(rows, d)

    return jax.shard_map(
        step,
        mesh=mesh,
        in_specs=(P("dp", None), P(None, "tp"), P(None, "tp"), P("tp", None)),
        out_specs=P("dp", None),
        check_vma=False,
    )
```

```python
import functools
import math

import jax
import jax.numpy as jnp
from jax import lax
from jax.experimental import pallas as pl
from jax.experimental.pallas import tpu as pltpu
from jax.sharding import PartitionSpec as P

MESH = pl.DeviceIdType.MESH
BLOCK = 256
HID0, OUT0 = 256, 1024
HID, OUT = 512, 1024
GROUPS = 4
SPLIT = 5


def kernel(side, x_hbm, wg_hbm, wu_hbm, wd_hbm, y, xb, wg, wu, wd, hid, term, own,
           s1s, s1r, s2s, s2r, s3s, s3r, s4s, s4r, x_sem, wg_sem, wu_sem, wd_sem,
           send_sem, recv_sem):
    rows, d = x_hbm.shape
    f = wg.shape[1]
    blocks = rows // BLOCK
    sec = BLOCK // side
    piece = sec // side
    h = sec // 2
    half = d // 2
    quarter = half // 2
    slots = term.shape[0]
    f32, bf16 = jnp.float32, jnp.bfloat16

    me = lax.axis_index("tp")
    i, j = me // side, me % side

    def up1(v):
        return lax.rem(v + 1, side)

    def dn1(v):
        return lax.rem(v + side - 1, side)

    def opp(v):
        return lax.rem(v + 2, side)

    along_x = (up1(i) * side + j, dn1(i) * side + j)
    along_y = (i * side + up1(j), i * side + dn1(j))
    first = (along_x, along_y)
    second = (along_y, along_x)
    pos = ((i, j), (j, i))

    barrier = pltpu.get_barrier_semaphore()
    for n in along_x + along_y:
        pl.semaphore_signal(barrier, inc=1, device_id={"tp": n}, device_id_type=MESH)

    def ds(start, size):
        return pl.ds(pl.multiple_of(start, size), size)

    def x_copy(b):
        return pltpu.make_async_copy(
            x_hbm.at[ds(b * BLOCK, BLOCK)], xb.at[lax.rem(b, 2)], x_sem.at[lax.rem(b, 2)])

    pieces0 = [(0, HID0), (HID0, HID0), (2 * HID0, f - 2 * HID0)]

    def load(src, dst, sem, n, first_col, size):
        cols = pl.ds(first_col, size)
        return pltpu.make_async_copy(src.at[:, cols], dst.at[:, cols], sem.at[n])

    def load_in(n):
        return load(wg_hbm, wg, wg_sem, n, *pieces0[n]), load(wu_hbm, wu, wu_sem, n, *pieces0[n])

    def load_out(n):
        return load(wd_hbm, wd, wd_sem, n, n * OUT0, OUT0)

    x_copy(0).start()
    for n in range(3):
        for c in load_in(n):
            c.start()

    def hidden(xs, first_col, size):
        cols = pl.ds(first_col, size)
        gate = jnp.dot(xb[xs], wg[:, cols], preferred_element_type=f32)
        up = jnp.dot(xb[xs], wu[:, cols], preferred_element_type=f32)
        hid[:, cols] = (jax.nn.gelu(gate) * up).astype(bf16)

    def down(slot, n, size):
        cols = pl.ds(n * size, size)
        term[slot, :, cols] = jnp.dot(hid[...], wd[:, cols], preferred_element_type=f32)

    def compute1(b):
        x_copy(b).wait()
        for n in range(f // HID):
            hidden(lax.rem(b, 2), n * HID, HID)

    def compute2(b):
        for n in range(d // OUT):
            down(lax.rem(b, slots), n, OUT)

        @pl.when(b + 2 < blocks)
        def _():
            x_copy(b + 2).start()

    def compute(b):
        compute1(b)
        compute2(b)

    def far(lo, n, t):
        bs = pl.ds(lo, n)
        return [(s1s.at[t, bs, pl.ds(w * h, h)], s1r.at[t, w, bs], first[t][w]) for w in range(2)]

    def near(lo, n, t):
        bs = pl.ds(lo, n)
        return [(s2s.at[t, w, bs], s2r.at[t, w, bs], first[t][w]) for w in range(2)]

    def near_part(b, t, own_half):
        k = [pl.ds((1 - w if own_half else w) * h, h) for w in range(2)]
        return [(s2s.at[t, w, b, k[w]], s2r.at[t, w, b, k[w]], first[t][w]) for w in range(2)]

    def far2(lo, n, t):
        bs = pl.ds(lo, n)
        return [(s3s.at[t, bs, :, pl.ds(w * quarter, quarter)], s3r.at[t, w, bs], second[t][w])
                for w in range(2)]

    def near2(lo, n, t):
        bs = pl.ds(lo, n)
        return [(s4s.at[t, w, bs], s4r.at[t, w, bs], second[t][w]) for w in range(2)]

    def gather1(lo, n, t):
        p, q = pos[t]
        at = y.at[pl.ds(lo, n), ds(p * sec + q * piece, piece), pl.ds(t * half, half)]
        return [(at, at, second[t][w]) for w in range(2)]

    def gather2(lo, n, t):
        p, q = pos[t]
        at = [y.at[pl.ds(lo, n), ds(p * sec + v * piece, piece),
                   pl.ds(t * half + w * quarter, quarter)] for w, v in enumerate((dn1(q), up1(q)))]
        return [(at[w], at[w], second[t][w]) for w in range(2)]

    def gather3(lo, n, t):
        p, _ = pos[t]
        at = y.at[pl.ds(lo, n), ds(p * sec, sec), pl.ds(t * half, half)]
        return [(at, at, first[t][w]) for w in range(2)]

    def gather4(lo, n, t):
        p, _ = pos[t]
        at = [y.at[pl.ds(lo, n), ds(v * sec + w * h, h), pl.ds(t * half, half)]
              for w, v in enumerate((dn1(p), up1(p)))]
        return [(at[w], at[w], first[t][w]) for w in range(2)]

    FAR, NEAR, FAR2, NEAR2 = 0, blocks, 2 * blocks, 2 * blocks + GROUPS
    OWN = NEAR2 + GROUPS
    LAST = OWN + SPLIT
    S_FAR, S_NEAR, S_FAR2, S_NEAR2 = range(4)

    def start(copies, sent, sem):
        for src, dst, to in copies:
            pltpu.make_async_remote_copy(
                src_ref=src, dst_ref=dst, send_sem=send_sem.at[sent], recv_sem=recv_sem.at[sem],
                device_id={"tp": to}, device_id_type=MESH).start()

    def arrive(like, sem):
        pltpu.make_async_copy(like, like, recv_sem.at[sem]).wait()

    def pack(lo, n, split, streams=range(2)):
        for t in streams:
            p, _ = pos[t]
            c = pl.ds(t * half, half)
            for k in range(n):
                s1s[t, lo + k] = term[lax.rem(lo + k, slots), ds(opp(p) * sec, sec), c].astype(bf16)
            start(far(lo, n, t), S_FAR, FAR + lo)
            for k in range(n):
                b = lo + k
                slot = lax.rem(b, slots)
                s2s[t, 0, b, pl.ds(h, h)] = term[slot, ds(up1(p) * sec + h, h), c].astype(bf16)
                s2s[t, 1, b, pl.ds(0, h)] = term[slot, ds(dn1(p) * sec, h), c].astype(bf16)
            if split:
                start(near_part(lo, t, True), S_NEAR, OWN + lo)

    def reduce1(lo, n, split):
        arrive(s1r.at[:, :, pl.ds(lo, n)], FAR + lo)
        for t in range(2):
            p, _ = pos[t]
            c = pl.ds(t * half, half)
            for k in range(n):
                b = lo + k
                slot = lax.rem(b, slots)
                s2s[t, 0, b, pl.ds(0, h)] = (
                    term[slot, ds(up1(p) * sec, h), c] + s1r[t, 0, b].astype(f32)).astype(bf16)
                s2s[t, 1, b, pl.ds(h, h)] = (
                    term[slot, ds(dn1(p) * sec + h, h), c] + s1r[t, 1, b].astype(f32)).astype(bf16)
            start(near_part(lo, t, False) if split else near(lo, n, t), S_NEAR, NEAR + lo)
        for t in range(2):
            p, _ = pos[t]
            for k in range(n):
                own[t, lo + k] = term[
                    lax.rem(lo + k, slots), ds(p * sec, sec), pl.ds(t * half, half)]

    def reduce2(g, lo, n):
        for b in range(lo, lo + n):
            if b < SPLIT:
                arrive(s1r.at[:, :, b], OWN + b)
                arrive(s1r.at[:, :, b], NEAR + b)
            else:
                arrive(s2r.at[:, :, b], NEAR + b)
        for t in range(2):
            _, q = pos[t]
            for b in range(lo, lo + n):
                own[t, b] = own[t, b] + s2r[t, 0, b].astype(f32) + s2r[t, 1, b].astype(f32)
                s3s[t, b] = own[t, b, ds(opp(q) * piece, piece), :].astype(bf16)
            start(far2(lo, n, t), S_FAR2, FAR2 + g)

    def reduce3(g, lo, n):
        left, right = pl.ds(0, quarter), pl.ds(quarter, quarter)
        arrive(s3r.at[:, :, pl.ds(lo, n)], FAR2 + g)
        for t in range(2):
            _, q = pos[t]
            r, l = ds(up1(q) * piece, piece), ds(dn1(q) * piece, piece)
            for b in range(lo, lo + n):
                s4s[t, 0, b, :, left] = (
                    own[t, b, r, left] + s3r[t, 0, b].astype(f32)).astype(bf16)
                s4s[t, 0, b, :, right] = own[t, b, r, right].astype(bf16)
                s4s[t, 1, b, :, left] = own[t, b, l, left].astype(bf16)
                s4s[t, 1, b, :, right] = (
                    own[t, b, l, right] + s3r[t, 1, b].astype(f32)).astype(bf16)
            start(near2(lo, n, t), S_NEAR2, NEAR2 + g)

    def g1_sem(g, lo):
        return FAR + lo + 1 if g < GROUPS - 1 else LAST

    def reduce4(g, lo, n):
        arrive(s4r.at[:, :, pl.ds(lo, n)], NEAR2 + g)
        for t in range(2):
            p, q = pos[t]
            for b in range(lo, lo + n):
                y[b, ds(p * sec + q * piece, piece), pl.ds(t * half, half)] = (
                    own[t, b, ds(q * piece, piece), :]
                    + s4r[t, 0, b].astype(f32) + s4r[t, 1, b].astype(f32)).astype(bf16)
            start(gather1(lo, n, t), S_NEAR2, g1_sem(g, lo))

    def send2(g, lo, n):
        arrive(s4r.at[:, :, pl.ds(lo, n)], g1_sem(g, lo))
        for t in range(2):
            start(gather2(lo, n, t), S_FAR2, FAR2 + g)

    def got2(g, lo, n):
        arrive(s3r.at[:, :, pl.ds(lo, n)], FAR2 + g)

    def send3(lo, n):
        for t in range(2):
            start(gather3(lo, n, t), S_NEAR, FAR + lo)

    def send4(lo, n):
        arrive(s2r.at[:, :, pl.ds(lo, n)], FAR + lo)
        for t in range(2):
            start(gather4(lo, n, t), S_FAR, NEAR + lo)

    def got4(lo, n):
        arrive(s1r.at[:, :, pl.ds(lo, n)], NEAR + lo)

    x_copy(0).wait()
    for n in range(3):
        for c in load_in(n):
            c.wait()
        if n == 1:
            for k in range(d // OUT0):
                load_out(k).start()
            x_copy(1).start()
        hidden(0, *pieces0[n])
    for t in range(2):
        for n in range(t * half // OUT0, (t + 1) * half // OUT0):
            load_out(n).wait()
            down(0, n, OUT0)
        if t == 0:
            pl.semaphore_wait(barrier, 4)
        pack(0, 1, True, (t,))
    x_copy(2).start()

    compute1(1)
    reduce1(0, 1, True)
    compute2(1)
    pack(1, 1, True)

    pair = [(g, 2 * g, 2) for g in range(GROUPS)]
    beside = {
        5: [(reduce2, *pair[0])],
        6: [(reduce2, *pair[1]), (reduce3, *pair[0])],
        7: [(reduce3, *pair[1]), (reduce4, *pair[0])],
    }

    def step(b, _):
        compute(b)

        @pl.when(b < SPLIT)
        def _():
            pack(b, 1, True)

        @pl.when(b >= SPLIT)
        def _():
            pack(b, 1, False)

        @pl.when(b <= SPLIT)
        def _():
            reduce1(b - 1, 1, True)

        @pl.when(b > SPLIT)
        def _():
            reduce1(b - 1, 1, False)

        for k, tasks in beside.items():
            @pl.when(b == k)
            def _():
                for task, *args in tasks:
                    task(*args)
        return 0

    lax.fori_loop(2, blocks, step, 0)

    for task, *args in [
        (reduce1, blocks - 1, 1, SPLIT == blocks),
        (reduce2, *pair[2]), (reduce4, *pair[1]), (send2, *pair[0]),
        (reduce3, *pair[2]), (reduce2, *pair[3]), (send2, *pair[1]),
        (got2, *pair[0]), (send3, 0, 2),
        (reduce4, *pair[2]), (reduce3, *pair[3]),
        (got2, *pair[1]), (send3, 2, 2),
        (send2, *pair[2]), (reduce4, *pair[3]),
        (got2, *pair[2]), (send3, 4, 2),
        (send2, *pair[3]), (send4, 0, 2),
        (got2, *pair[3]), (send3, 6, 1), (send3, 7, 1),
        (send4, 2, 2), (send4, 4, 2), (send4, 6, 1), (send4, 7, 1),
        (got4, 0, 2), (got4, 2, 2), (got4, 4, 2), (got4, 6, 1), (got4, 7, 1),
    ]:
        task(*args)

    for sent, like in enumerate((s2s, y, s4s, s1s)):
        pltpu.make_async_copy(like, like, send_sem.at[sent]).wait()


def solution(mesh):
    side = math.isqrt(mesh.shape["tp"])

    def step(x, w_gate, w_up, w_down):
        rows, d = x.shape
        f = w_gate.shape[1]
        blocks, sec = rows // BLOCK, BLOCK // side
        piece, half = sec // side, d // 2
        bf16, f32 = jnp.bfloat16, jnp.float32
        return pl.pallas_call(
            functools.partial(kernel, side),
            out_shape=pltpu.VMEM((blocks, BLOCK, d), bf16),
            in_specs=[pl.BlockSpec(memory_space=pl.ANY)] * 4,
            out_specs=pl.BlockSpec(memory_space=pltpu.VMEM),
            scratch_shapes=[
                pltpu.VMEM((2, BLOCK, d), bf16),
                pltpu.VMEM((d, f), bf16),
                pltpu.VMEM((d, f), bf16),
                pltpu.VMEM((f, d), bf16),
                pltpu.VMEM((BLOCK, f), bf16),
                pltpu.VMEM((4, BLOCK, d), f32),
                pltpu.VMEM((2, blocks, sec, half), f32),
                pltpu.VMEM((2, blocks, sec, half), bf16),
                pltpu.VMEM((2, 2, blocks, sec // 2, half), bf16),
                pltpu.VMEM((2, 2, blocks, sec, half), bf16),
                pltpu.VMEM((2, 2, blocks, sec, half), bf16),
                pltpu.VMEM((2, blocks, piece, half), bf16),
                pltpu.VMEM((2, 2, blocks, piece, half // 2), bf16),
                pltpu.VMEM((2, 2, blocks, piece, half), bf16),
                pltpu.VMEM((2, 2, blocks, piece, half), bf16),
                pltpu.SemaphoreType.DMA((2,)),
                pltpu.SemaphoreType.DMA((3,)),
                pltpu.SemaphoreType.DMA((3,)),
                pltpu.SemaphoreType.DMA((d // OUT0,)),
                pltpu.SemaphoreType.DMA((4,)),
                pltpu.SemaphoreType.DMA((2 * blocks + 2 * GROUPS + SPLIT + 1,)),
            ],
            compiler_params=pltpu.CompilerParams(
                collective_id=0, has_side_effects=True, vmem_limit_bytes=50 * 2**20),
        )(x, w_gate, w_up, w_down).reshape(rows, d)

    return jax.shard_map(
        step,
        mesh=mesh,
        in_specs=(P("dp", None), P(None, "tp"), P(None, "tp"), P("tp", None)),
        out_specs=P("dp", None),
        check_vma=False,
    )
```

```python
import functools
import math

import jax
import jax.numpy as jnp
from jax import lax
from jax.experimental import pallas as pl
from jax.experimental.pallas import tpu as pltpu
from jax.sharding import PartitionSpec as P

MESH = pl.DeviceIdType.MESH
BLOCK = 256
HID0, OUT0 = 256, 1024
HID, OUT = 512, 1024
GROUPS = 4


def kernel(side, x_hbm, wg_hbm, wu_hbm, wd_hbm, y, xb, wg, wu, wd, hid, term, own,
           s1s, s1r, s2s, s2r, s3s, s3r, s4s, s4r, x_sem, wg_sem, wu_sem, wd_sem,
           send_sem, recv_sem):
    rows, d = x_hbm.shape
    f = wg.shape[1]
    blocks = rows // BLOCK
    sec = BLOCK // side
    piece = sec // side
    h = sec // 2
    half = d // 2
    quarter = half // 2
    slots = term.shape[0]
    f32, bf16 = jnp.float32, jnp.bfloat16

    me = lax.axis_index("tp")
    i, j = me // side, me % side

    def up1(v):
        return lax.rem(v + 1, side)

    def dn1(v):
        return lax.rem(v + side - 1, side)

    def opp(v):
        return lax.rem(v + 2, side)

    along_x = (up1(i) * side + j, dn1(i) * side + j)
    along_y = (i * side + up1(j), i * side + dn1(j))
    first = (along_x, along_y)
    second = (along_y, along_x)
    pos = ((i, j), (j, i))

    barrier = pltpu.get_barrier_semaphore()
    for n in along_x + along_y:
        pl.semaphore_signal(barrier, inc=1, device_id={"tp": n}, device_id_type=MESH)

    def ds(start, size):
        return pl.ds(pl.multiple_of(start, size), size)

    def x_copy(b):
        return pltpu.make_async_copy(
            x_hbm.at[ds(b * BLOCK, BLOCK)], xb.at[lax.rem(b, 2)], x_sem.at[lax.rem(b, 2)])

    pieces0 = [(0, HID0), (HID0, HID0), (2 * HID0, f - 2 * HID0)]

    def load(src, dst, sem, n, first_col, size):
        cols = pl.ds(first_col, size)
        return pltpu.make_async_copy(src.at[:, cols], dst.at[:, cols], sem.at[n])

    def load_in(n):
        return load(wg_hbm, wg, wg_sem, n, *pieces0[n]), load(wu_hbm, wu, wu_sem, n, *pieces0[n])

    def load_out(n):
        return load(wd_hbm, wd, wd_sem, n, n * OUT0, OUT0)

    x_copy(0).start()
    for n in range(3):
        for c in load_in(n):
            c.start()

    def hidden(xs, first_col, size):
        cols = pl.ds(first_col, size)
        gate = jnp.dot(xb[xs], wg[:, cols], preferred_element_type=f32)
        up = jnp.dot(xb[xs], wu[:, cols], preferred_element_type=f32)
        hid[:, cols] = (jax.nn.gelu(gate) * up).astype(bf16)

    def down(slot, n, size):
        cols = pl.ds(n * size, size)
        term[slot, :, cols] = jnp.dot(hid[...], wd[:, cols], preferred_element_type=f32)

    def compute1(b):
        x_copy(b).wait()
        for n in range(f // HID):
            hidden(lax.rem(b, 2), n * HID, HID)

    def compute2(b, t):
        for n in range(t * half // OUT, (t + 1) * half // OUT):
            down(lax.rem(b, slots), n, OUT)
        pack(b, t)

    def next_rows(b):
        @pl.when(b + 2 < blocks)
        def _():
            x_copy(b + 2).start()

    def far(b, t):
        return [(s1s.at[t, b, pl.ds(w * h, h)], s1r.at[t, w, b], first[t][w]) for w in range(2)]

    def near(b, t, own_half):
        k = [pl.ds((1 - w if own_half else w) * h, h) for w in range(2)]
        return [(s2s.at[t, w, b, k[w]], s2r.at[t, w, b, k[w]], first[t][w]) for w in range(2)]

    def far2(lo, n, t):
        bs = pl.ds(lo, n)
        return [(s3s.at[t, bs, :, pl.ds(w * quarter, quarter)], s3r.at[t, w, bs], second[t][w])
                for w in range(2)]

    def near2(lo, n, t):
        bs = pl.ds(lo, n)
        return [(s4s.at[t, w, bs], s4r.at[t, w, bs], second[t][w]) for w in range(2)]

    def gather1(lo, n, t):
        p, q = pos[t]
        at = y.at[pl.ds(lo, n), ds(p * sec + q * piece, piece), pl.ds(t * half, half)]
        return [(at, at, second[t][w]) for w in range(2)]

    def gather2(lo, n, t):
        p, q = pos[t]
        at = [y.at[pl.ds(lo, n), ds(p * sec + v * piece, piece),
                   pl.ds(t * half + w * quarter, quarter)] for w, v in enumerate((dn1(q), up1(q)))]
        return [(at[w], at[w], second[t][w]) for w in range(2)]

    def gather3(lo, n, t):
        p, _ = pos[t]
        at = y.at[pl.ds(lo, n), ds(p * sec, sec), pl.ds(t * half, half)]
        return [(at, at, first[t][w]) for w in range(2)]

    def gather4(lo, n, t):
        p, _ = pos[t]
        at = [y.at[pl.ds(lo, n), ds(v * sec + w * h, h), pl.ds(t * half, half)]
              for w, v in enumerate((dn1(p), up1(p)))]
        return [(at[w], at[w], first[t][w]) for w in range(2)]

    FAR, NEAR, FAR2, NEAR2 = 0, blocks, 2 * blocks, 2 * blocks + GROUPS
    OWN = NEAR2 + GROUPS
    LAST = OWN + blocks
    S_FAR, S_NEAR, S_FAR2, S_NEAR2 = range(4)

    def start(copies, sent, sem):
        for src, dst, to in copies:
            pltpu.make_async_remote_copy(
                src_ref=src, dst_ref=dst, send_sem=send_sem.at[sent], recv_sem=recv_sem.at[sem],
                device_id={"tp": to}, device_id_type=MESH).start()

    def arrive(like, sem):
        pltpu.make_async_copy(like, like, recv_sem.at[sem]).wait()

    def pack(b, t):
        slot = lax.rem(b, slots)
        p, _ = pos[t]
        c = pl.ds(t * half, half)
        s1s[t, b] = term[slot, ds(opp(p) * sec, sec), c].astype(bf16)
        start(far(b, t), S_FAR, FAR + b)
        s2s[t, 0, b, pl.ds(h, h)] = term[slot, ds(up1(p) * sec + h, h), c].astype(bf16)
        s2s[t, 1, b, pl.ds(0, h)] = term[slot, ds(dn1(p) * sec, h), c].astype(bf16)
        start(near(b, t, True), S_NEAR, OWN + b)

    def reduce1(b):
        slot = lax.rem(b, slots)
        arrive(s1r.at[:, :, b], FAR + b)
        for t in range(2):
            p, _ = pos[t]
            c = pl.ds(t * half, half)
            s2s[t, 0, b, pl.ds(0, h)] = (
                term[slot, ds(up1(p) * sec, h), c] + s1r[t, 0, b].astype(f32)).astype(bf16)
            s2s[t, 1, b, pl.ds(h, h)] = (
                term[slot, ds(dn1(p) * sec + h, h), c] + s1r[t, 1, b].astype(f32)).astype(bf16)
            start(near(b, t, False), S_NEAR, NEAR + b)
        for t in range(2):
            p, _ = pos[t]
            own[t, b] = term[slot, ds(p * sec, sec), pl.ds(t * half, half)]

    def reduce2(g, lo, n):
        for b in range(lo, lo + n):
            arrive(s1r.at[:, :, b], OWN + b)
            arrive(s1r.at[:, :, b], NEAR + b)
        for t in range(2):
            _, q = pos[t]
            for b in range(lo, lo + n):
                own[t, b] = own[t, b] + s2r[t, 0, b].astype(f32) + s2r[t, 1, b].astype(f32)
                s3s[t, b] = own[t, b, ds(opp(q) * piece, piece), :].astype(bf16)
            start(far2(lo, n, t), S_FAR2, FAR2 + g)

    def reduce3(g, lo, n):
        left, right = pl.ds(0, quarter), pl.ds(quarter, quarter)
        arrive(s3r.at[:, :, pl.ds(lo, n)], FAR2 + g)
        for t in range(2):
            _, q = pos[t]
            r, l = ds(up1(q) * piece, piece), ds(dn1(q) * piece, piece)
            for b in range(lo, lo + n):
                s4s[t, 0, b, :, left] = (
                    own[t, b, r, left] + s3r[t, 0, b].astype(f32)).astype(bf16)
                s4s[t, 0, b, :, right] = own[t, b, r, right].astype(bf16)
                s4s[t, 1, b, :, left] = own[t, b, l, left].astype(bf16)
                s4s[t, 1, b, :, right] = (
                    own[t, b, l, right] + s3r[t, 1, b].astype(f32)).astype(bf16)
            start(near2(lo, n, t), S_NEAR2, NEAR2 + g)

    def g1_sem(g, lo):
        return FAR + lo + 1 if g < GROUPS - 1 else LAST

    def reduce4(g, lo, n):
        arrive(s4r.at[:, :, pl.ds(lo, n)], NEAR2 + g)
        for t in range(2):
            p, q = pos[t]
            for b in range(lo, lo + n):
                y[b, ds(p * sec + q * piece, piece), pl.ds(t * half, half)] = (
                    own[t, b, ds(q * piece, piece), :]
                    + s4r[t, 0, b].astype(f32) + s4r[t, 1, b].astype(f32)).astype(bf16)
            start(gather1(lo, n, t), S_NEAR2, g1_sem(g, lo))

    def send2(g, lo, n):
        arrive(s4r.at[:, :, pl.ds(lo, n)], g1_sem(g, lo))
        for t in range(2):
            start(gather2(lo, n, t), S_FAR2, FAR2 + g)

    def got2(g, lo, n):
        arrive(s3r.at[:, :, pl.ds(lo, n)], FAR2 + g)

    def send3(lo, n):
        for t in range(2):
            start(gather3(lo, n, t), S_NEAR, FAR + lo)

    def send4(lo, n):
        arrive(s2r.at[:, :, pl.ds(lo, n)], FAR + lo)
        for t in range(2):
            start(gather4(lo, n, t), S_FAR, NEAR + lo)

    def got4(lo, n):
        arrive(s1r.at[:, :, pl.ds(lo, n)], NEAR + lo)

    x_copy(0).wait()
    for n in range(3):
        for c in load_in(n):
            c.wait()
        if n == 1:
            for k in range(d // OUT0):
                load_out(k).start()
            x_copy(1).start()
        hidden(0, *pieces0[n])
    for t in range(2):
        for n in range(t * half // OUT0, (t + 1) * half // OUT0):
            load_out(n).wait()
            down(0, n, OUT0)
        if t == 0:
            pl.semaphore_wait(barrier, 4)
        pack(0, t)
    x_copy(2).start()

    compute1(1)
    compute2(1, 0)
    reduce1(0)
    compute2(1, 1)
    next_rows(1)

    pair = [(g, 2 * g, 2) for g in range(GROUPS)]
    beside = {
        5: [(reduce2, *pair[0])],
        6: [(reduce2, *pair[1]), (reduce3, *pair[0])],
        7: [(reduce3, *pair[1]), (reduce4, *pair[0])],
    }

    def step(b, _):
        compute1(b)
        compute2(b, 0)
        compute2(b, 1)
        next_rows(b)
        reduce1(b - 1)

        for k, tasks in beside.items():
            @pl.when(b == k)
            def _():
                for task, *args in tasks:
                    task(*args)
        return 0

    lax.fori_loop(2, blocks, step, 0)

    for task, *args in [
        (reduce1, blocks - 1),
        (reduce2, *pair[2]), (reduce4, *pair[1]), (send2, *pair[0]),
        (reduce3, *pair[2]), (reduce2, *pair[3]), (send2, *pair[1]),
        (got2, *pair[0]), (send3, 0, 2),
        (reduce4, *pair[2]), (reduce3, *pair[3]),
        (got2, *pair[1]), (send3, 2, 2),
        (send2, *pair[2]), (reduce4, *pair[3]),
        (got2, *pair[2]), (send3, 4, 2),
        (send2, *pair[3]), (send4, 0, 2),
        (got2, *pair[3]), (send3, 6, 1), (send3, 7, 1),
        (send4, 2, 2), (send4, 4, 2), (send4, 6, 1), (send4, 7, 1),
        (got4, 0, 2), (got4, 2, 2), (got4, 4, 2), (got4, 6, 1), (got4, 7, 1),
    ]:
        task(*args)

    for sent, like in enumerate((s2s, y, s4s, s1s)):
        pltpu.make_async_copy(like, like, send_sem.at[sent]).wait()


def solution(mesh):
    side = math.isqrt(mesh.shape["tp"])

    def step(x, w_gate, w_up, w_down):
        rows, d = x.shape
        f = w_gate.shape[1]
        blocks, sec = rows // BLOCK, BLOCK // side
        piece, half = sec // side, d // 2
        bf16, f32 = jnp.bfloat16, jnp.float32
        return pl.pallas_call(
            functools.partial(kernel, side),
            out_shape=pltpu.VMEM((blocks, BLOCK, d), bf16),
            in_specs=[pl.BlockSpec(memory_space=pl.ANY)] * 4,
            out_specs=pl.BlockSpec(memory_space=pltpu.VMEM),
            scratch_shapes=[
                pltpu.VMEM((2, BLOCK, d), bf16),
                pltpu.VMEM((d, f), bf16),
                pltpu.VMEM((d, f), bf16),
                pltpu.VMEM((f, d), bf16),
                pltpu.VMEM((BLOCK, f), bf16),
                pltpu.VMEM((4, BLOCK, d), f32),
                pltpu.VMEM((2, blocks, sec, half), f32),
                pltpu.VMEM((2, blocks, sec, half), bf16),
                pltpu.VMEM((2, 2, blocks, sec // 2, half), bf16),
                pltpu.VMEM((2, 2, blocks, sec, half), bf16),
                pltpu.VMEM((2, 2, blocks, sec, half), bf16),
                pltpu.VMEM((2, blocks, piece, half), bf16),
                pltpu.VMEM((2, 2, blocks, piece, half // 2), bf16),
                pltpu.VMEM((2, 2, blocks, piece, half), bf16),
                pltpu.VMEM((2, 2, blocks, piece, half), bf16),
                pltpu.SemaphoreType.DMA((2,)),
                pltpu.SemaphoreType.DMA((3,)),
                pltpu.SemaphoreType.DMA((3,)),
                pltpu.SemaphoreType.DMA((d // OUT0,)),
                pltpu.SemaphoreType.DMA((4,)),
                pltpu.SemaphoreType.DMA((3 * blocks + 2 * GROUPS + 1,)),
            ],
            compiler_params=pltpu.CompilerParams(
                collective_id=0, has_side_effects=True, vmem_limit_bytes=50 * 2**20),
        )(x, w_gate, w_up, w_down).reshape(rows, d)

    return jax.shard_map(
        step,
        mesh=mesh,
        in_specs=(P("dp", None), P(None, "tp"), P(None, "tp"), P("tp", None)),
        out_specs=P("dp", None),
        check_vma=False,
    )
```

```python
import functools
import math

import jax
import jax.numpy as jnp
from jax import lax
from jax.experimental import pallas as pl
from jax.experimental.pallas import tpu as pltpu
from jax.sharding import PartitionSpec as P

MESH = pl.DeviceIdType.MESH
BLOCK = 256
HID0, OUT0 = 256, 1024
HID, OUT = 512, 1024


def kernel(side, x_hbm, wg_hbm, wu_hbm, wd_hbm, y, xb, wg, wu, wd, hid, term, own,
           s1s, s1r, s2s, s2r, s3s, s3r, s4s, s4r, x_sem, wg_sem, wu_sem, wd_sem,
           send_sem, recv_sem):
    rows, d = x_hbm.shape
    f = wg.shape[1]
    blocks = rows // BLOCK
    sec = BLOCK // side
    piece = sec // side
    h = sec // 2
    half = d // 2
    quarter = half // 2
    slots = term.shape[0]
    f32, bf16 = jnp.float32, jnp.bfloat16

    me = lax.axis_index("tp")
    i, j = me // side, me % side

    def up1(v):
        return lax.rem(v + 1, side)

    def dn1(v):
        return lax.rem(v + side - 1, side)

    def opp(v):
        return lax.rem(v + 2, side)

    along_x = (up1(i) * side + j, dn1(i) * side + j)
    along_y = (i * side + up1(j), i * side + dn1(j))
    first = (along_x, along_y)
    second = (along_y, along_x)
    pos = ((i, j), (j, i))

    barrier = pltpu.get_barrier_semaphore()
    for n in along_x + along_y:
        pl.semaphore_signal(barrier, inc=1, device_id={"tp": n}, device_id_type=MESH)

    def ds(start, size):
        return pl.ds(pl.multiple_of(start, size), size)

    def x_copy(b):
        return pltpu.make_async_copy(
            x_hbm.at[ds(b * BLOCK, BLOCK)], xb.at[lax.rem(b, 2)], x_sem.at[lax.rem(b, 2)])

    pieces0 = [(0, HID0), (HID0, HID0), (2 * HID0, f - 2 * HID0)]

    def load(src, dst, sem, n, first_col, size):
        cols = pl.ds(first_col, size)
        return pltpu.make_async_copy(src.at[:, cols], dst.at[:, cols], sem.at[n])

    def load_in(n):
        return load(wg_hbm, wg, wg_sem, n, *pieces0[n]), load(wu_hbm, wu, wu_sem, n, *pieces0[n])

    def load_out(n):
        return load(wd_hbm, wd, wd_sem, n, n * OUT0, OUT0)

    x_copy(0).start()
    for n in range(3):
        for c in load_in(n):
            c.start()

    def hidden(xs, first_col, size):
        cols = pl.ds(first_col, size)
        gate = jnp.dot(xb[xs], wg[:, cols], preferred_element_type=f32)
        up = jnp.dot(xb[xs], wu[:, cols], preferred_element_type=f32)
        hid[:, cols] = (jax.nn.gelu(gate) * up).astype(bf16)

    def down(slot, n, size):
        cols = pl.ds(n * size, size)
        term[slot, :, cols] = jnp.dot(hid[...], wd[:, cols], preferred_element_type=f32)

    def compute1(b):
        x_copy(b).wait()
        for n in range(f // HID):
            hidden(lax.rem(b, 2), n * HID, HID)

    def compute2(b, t):
        for n in range(t * half // OUT, (t + 1) * half // OUT):
            down(lax.rem(b, slots), n, OUT)
        pack(b, t)

    def next_rows(b):
        @pl.when(b + 2 < blocks)
        def _():
            x_copy(b + 2).start()

    def far(b, t):
        return [(s1s.at[t, b, pl.ds(w * h, h)], s1r.at[t, w, b], first[t][w]) for w in range(2)]

    def near(b, t, own_half):
        k = [pl.ds((1 - w if own_half else w) * h, h) for w in range(2)]
        return [(s2s.at[t, w, b, k[w]], s2r.at[t, w, b, k[w]], first[t][w]) for w in range(2)]

    def far2(lo, n, t):
        bs = pl.ds(lo, n)
        return [(s3s.at[t, bs, :, pl.ds(w * quarter, quarter)], s3r.at[t, w, bs], second[t][w])
                for w in range(2)]

    def near2(lo, n, t):
        bs = pl.ds(lo, n)
        return [(s4s.at[t, w, bs], s4r.at[t, w, bs], second[t][w]) for w in range(2)]

    def gather1(lo, n, t):
        p, q = pos[t]
        at = y.at[pl.ds(lo, n), ds(p * sec + q * piece, piece), pl.ds(t * half, half)]
        return [(at, at, second[t][w]) for w in range(2)]

    def gather2(lo, n, t):
        p, q = pos[t]
        at = [y.at[pl.ds(lo, n), ds(p * sec + v * piece, piece),
                   pl.ds(t * half + w * quarter, quarter)] for w, v in enumerate((dn1(q), up1(q)))]
        return [(at[w], at[w], second[t][w]) for w in range(2)]

    def gather3(lo, n, t):
        p, _ = pos[t]
        at = y.at[pl.ds(lo, n), ds(p * sec, sec), pl.ds(t * half, half)]
        return [(at, at, first[t][w]) for w in range(2)]

    def gather4(lo, n, t):
        p, _ = pos[t]
        at = [y.at[pl.ds(lo, n), ds(v * sec + w * h, h), pl.ds(t * half, half)]
              for w, v in enumerate((dn1(p), up1(p)))]
        return [(at[w], at[w], first[t][w]) for w in range(2)]

    FAR, NEAR = 0, blocks
    S_FAR, S_NEAR, S_FAR2, S_NEAR2 = range(4)

    def start(copies, sent, sem):
        for src, dst, to in copies:
            pltpu.make_async_remote_copy(
                src_ref=src, dst_ref=dst, send_sem=send_sem.at[sent], recv_sem=recv_sem.at[sem],
                device_id={"tp": to}, device_id_type=MESH).start()

    def arrive(like, sem):
        pltpu.make_async_copy(like, like, recv_sem.at[sem]).wait()

    def pack(b, t):
        slot = lax.rem(b, slots)
        p, _ = pos[t]
        c = pl.ds(t * half, half)
        s1s[t, b] = term[slot, ds(opp(p) * sec, sec), c].astype(bf16)
        start(far(b, t), S_FAR, FAR + b)
        s2s[t, 0, b, pl.ds(h, h)] = term[slot, ds(up1(p) * sec + h, h), c].astype(bf16)
        s2s[t, 1, b, pl.ds(0, h)] = term[slot, ds(dn1(p) * sec, h), c].astype(bf16)
        start(near(b, t, True), S_NEAR, NEAR + b)

    def reduce1(b):
        slot = lax.rem(b, slots)
        arrive(s1r.at[:, :, b], FAR + b)
        for t in range(2):
            p, _ = pos[t]
            c = pl.ds(t * half, half)
            s2s[t, 0, b, pl.ds(0, h)] = (
                term[slot, ds(up1(p) * sec, h), c] + s1r[t, 0, b].astype(f32)).astype(bf16)
            s2s[t, 1, b, pl.ds(h, h)] = (
                term[slot, ds(dn1(p) * sec + h, h), c] + s1r[t, 1, b].astype(f32)).astype(bf16)
            start(near(b, t, False), S_NEAR, NEAR + b)
        for t in range(2):
            p, _ = pos[t]
            own[t, b] = term[slot, ds(p * sec, sec), pl.ds(t * half, half)]

    def reduce2(lo, n):
        for b in range(lo, lo + n):
            arrive(s2r.at[:, :, b], NEAR + b)
        for t in range(2):
            _, q = pos[t]
            for b in range(lo, lo + n):
                own[t, b] = own[t, b] + s2r[t, 0, b].astype(f32) + s2r[t, 1, b].astype(f32)
                s3s[t, b] = own[t, b, ds(opp(q) * piece, piece), :].astype(bf16)
            start(far2(lo, n, t), S_FAR2, FAR + lo + 1)

    def reduce3(lo, n):
        left, right = pl.ds(0, quarter), pl.ds(quarter, quarter)
        arrive(s3r.at[:, :, pl.ds(lo, n)], FAR + lo + 1)
        for t in range(2):
            _, q = pos[t]
            r, l = ds(up1(q) * piece, piece), ds(dn1(q) * piece, piece)
            for b in range(lo, lo + n):
                s4s[t, 0, b, :, left] = (
                    own[t, b, r, left] + s3r[t, 0, b].astype(f32)).astype(bf16)
                s4s[t, 0, b, :, right] = own[t, b, r, right].astype(bf16)
                s4s[t, 1, b, :, left] = own[t, b, l, left].astype(bf16)
                s4s[t, 1, b, :, right] = (
                    own[t, b, l, right] + s3r[t, 1, b].astype(f32)).astype(bf16)
            start(near2(lo, n, t), S_NEAR2, NEAR + lo + 1)

    def reduce4(lo, n):
        arrive(s4r.at[:, :, pl.ds(lo, n)], NEAR + lo + 1)
        for t in range(2):
            p, q = pos[t]
            for b in range(lo, lo + n):
                y[b, ds(p * sec + q * piece, piece), pl.ds(t * half, half)] = (
                    own[t, b, ds(q * piece, piece), :]
                    + s4r[t, 0, b].astype(f32) + s4r[t, 1, b].astype(f32)).astype(bf16)
            start(gather1(lo, n, t), S_NEAR2, FAR + lo + 1)

    def send2(lo, n):
        arrive(s4r.at[:, :, pl.ds(lo, n)], FAR + lo + 1)
        for t in range(2):
            start(gather2(lo, n, t), S_FAR2, NEAR + lo + 1)

    def got2(lo, n):
        arrive(s3r.at[:, :, pl.ds(lo, n)], NEAR + lo + 1)

    def send3(lo, n):
        for t in range(2):
            start(gather3(lo, n, t), S_NEAR, FAR + lo)

    def send4(lo, n):
        arrive(s2r.at[:, :, pl.ds(lo, n)], FAR + lo)
        for t in range(2):
            start(gather4(lo, n, t), S_FAR, NEAR + lo)

    def got4(lo, n):
        arrive(s1r.at[:, :, pl.ds(lo, n)], NEAR + lo)

    x_copy(0).wait()
    for n in range(3):
        for c in load_in(n):
            c.wait()
        if n == 1:
            for k in range(d // OUT0):
                load_out(k).start()
            x_copy(1).start()
        hidden(0, *pieces0[n])
    for t in range(2):
        for n in range(t * half // OUT0, (t + 1) * half // OUT0):
            load_out(n).wait()
            down(0, n, OUT0)
        if t == 0:
            pl.semaphore_wait(barrier, 4)
        pack(0, t)
    x_copy(2).start()

    compute1(1)
    compute2(1, 0)
    reduce1(0)
    compute2(1, 1)
    next_rows(1)

    pair = [(b, 2) for b in range(0, blocks, 2)]
    beside = {
        5: [(reduce2, *pair[0])],
        6: [(reduce2, *pair[1]), (reduce3, *pair[0])],
        7: [(reduce3, *pair[1]), (reduce4, *pair[0])],
    }

    def step(b, _):
        compute1(b)
        compute2(b, 0)
        compute2(b, 1)
        next_rows(b)
        reduce1(b - 1)

        for k, tasks in beside.items():
            @pl.when(b == k)
            def _():
                for task, *args in tasks:
                    task(*args)
        return 0

    lax.fori_loop(2, blocks, step, 0)

    for task, *args in [
        (reduce1, blocks - 1),
        (reduce2, *pair[2]), (reduce4, *pair[1]), (send2, *pair[0]),
        (reduce3, *pair[2]), (reduce2, *pair[3]), (send2, *pair[1]),
        (got2, *pair[0]), (send3, 0, 2),
        (reduce4, *pair[2]), (reduce3, *pair[3]),
        (got2, *pair[1]), (send3, 2, 2),
        (send2, *pair[2]), (reduce4, *pair[3]),
        (got2, *pair[2]), (send3, 4, 2),
        (send2, *pair[3]), (send4, 0, 2),
        (got2, *pair[3]), (send3, 6, 1), (send3, 7, 1),
        (send4, 2, 2), (send4, 4, 2), (send4, 6, 1), (send4, 7, 1),
        (got4, 0, 2), (got4, 2, 2), (got4, 4, 2), (got4, 6, 1), (got4, 7, 1),
    ]:
        task(*args)

    for sent, like in enumerate((s2s, y, s4s, s1s)):
        pltpu.make_async_copy(like, like, send_sem.at[sent]).wait()


def solution(mesh):
    side = math.isqrt(mesh.shape["tp"])

    def step(x, w_gate, w_up, w_down):
        rows, d = x.shape
        f = w_gate.shape[1]
        blocks, sec = rows // BLOCK, BLOCK // side
        piece, half = sec // side, d // 2
        bf16, f32 = jnp.bfloat16, jnp.float32
        return pl.pallas_call(
            functools.partial(kernel, side),
            out_shape=pltpu.VMEM((blocks, BLOCK, d), bf16),
            in_specs=[pl.BlockSpec(memory_space=pl.ANY)] * 4,
            out_specs=pl.BlockSpec(memory_space=pltpu.VMEM),
            scratch_shapes=[
                pltpu.VMEM((2, BLOCK, d), bf16),
                pltpu.VMEM((d, f), bf16),
                pltpu.VMEM((d, f), bf16),
                pltpu.VMEM((f, d), bf16),
                pltpu.VMEM((BLOCK, f), bf16),
                pltpu.VMEM((4, BLOCK, d), f32),
                pltpu.VMEM((2, blocks, sec, half), f32),
                pltpu.VMEM((2, blocks, sec, half), bf16),
                pltpu.VMEM((2, 2, blocks, sec // 2, half), bf16),
                pltpu.VMEM((2, 2, blocks, sec, half), bf16),
                pltpu.VMEM((2, 2, blocks, sec, half), bf16),
                pltpu.VMEM((2, blocks, piece, half), bf16),
                pltpu.VMEM((2, 2, blocks, piece, half // 2), bf16),
                pltpu.VMEM((2, 2, blocks, piece, half), bf16),
                pltpu.VMEM((2, 2, blocks, piece, half), bf16),
                pltpu.SemaphoreType.DMA((2,)),
                pltpu.SemaphoreType.DMA((3,)),
                pltpu.SemaphoreType.DMA((3,)),
                pltpu.SemaphoreType.DMA((d // OUT0,)),
                pltpu.SemaphoreType.DMA((4,)),
                pltpu.SemaphoreType.DMA((2 * blocks,)),
            ],
            compiler_params=pltpu.CompilerParams(
                collective_id=0, has_side_effects=True, vmem_limit_bytes=50 * 2**20),
        )(x, w_gate, w_up, w_down).reshape(rows, d)

    return jax.shard_map(
        step,
        mesh=mesh,
        in_specs=(P("dp", None), P(None, "tp"), P(None, "tp"), P("tp", None)),
        out_specs=P("dp", None),
        check_vma=False,
    )
```

```python
import functools
import math

import jax
import jax.numpy as jnp
from jax import lax
from jax.experimental import pallas as pl
from jax.experimental.pallas import tpu as pltpu
from jax.sharding import PartitionSpec as P

MESH = pl.DeviceIdType.MESH
BLOCK = 256
HID0, OUT0 = 256, 1024
HID, OUT = 1024, 1024


def kernel(side, x_hbm, wg_hbm, wu_hbm, wd_hbm, y, xb, wg, wu, wd, hid, term, own,
           s1s, s1r, s2s, s2r, s3s, s3r, s4s, s4r, x_sem, wg_sem, wu_sem, wd_sem,
           send_sem, recv_sem):
    rows, d = x_hbm.shape
    f = wg.shape[1]
    blocks = rows // BLOCK
    sec = BLOCK // side
    piece = sec // side
    h = sec // 2
    half = d // 2
    quarter = half // 2
    slots = term.shape[0]
    f32, bf16 = jnp.float32, jnp.bfloat16

    me = lax.axis_index("tp")
    i, j = me // side, me % side

    def up1(v):
        return lax.rem(v + 1, side)

    def dn1(v):
        return lax.rem(v + side - 1, side)

    def opp(v):
        return lax.rem(v + 2, side)

    along_x = (up1(i) * side + j, dn1(i) * side + j)
    along_y = (i * side + up1(j), i * side + dn1(j))
    first = (along_x, along_y)
    second = (along_y, along_x)
    pos = ((i, j), (j, i))

    barrier = pltpu.get_barrier_semaphore()
    for n in along_x + along_y:
        pl.semaphore_signal(barrier, inc=1, device_id={"tp": n}, device_id_type=MESH)

    def ds(start, size):
        return pl.ds(pl.multiple_of(start, size), size)

    def x_copy(b):
        return pltpu.make_async_copy(
            x_hbm.at[ds(b * BLOCK, BLOCK)], xb.at[lax.rem(b, 2)], x_sem.at[lax.rem(b, 2)])

    pieces0 = [(0, HID0), (HID0, HID0), (2 * HID0, f - 2 * HID0)]

    def load(src, dst, sem, n, first_col, size):
        cols = pl.ds(first_col, size)
        return pltpu.make_async_copy(src.at[:, cols], dst.at[:, cols], sem.at[n])

    def load_in(n):
        return load(wg_hbm, wg, wg_sem, n, *pieces0[n]), load(wu_hbm, wu, wu_sem, n, *pieces0[n])

    def load_out(n):
        return load(wd_hbm, wd, wd_sem, n, n * OUT0, OUT0)

    x_copy(0).start()
    for n in range(3):
        for c in load_in(n):
            c.start()

    def hidden(xs, first_col, size):
        cols = pl.ds(first_col, size)
        gate = jnp.dot(xb[xs], wg[:, cols], preferred_element_type=f32)
        up = jnp.dot(xb[xs], wu[:, cols], preferred_element_type=f32)
        hid[:, cols] = (jax.nn.gelu(gate) * up).astype(bf16)

    def down(slot, n, size):
        cols = pl.ds(n * size, size)
        term[slot, :, cols] = jnp.dot(hid[...], wd[:, cols], preferred_element_type=f32)

    def compute1(b):
        x_copy(b).wait()
        for n in range(f // HID):
            hidden(lax.rem(b, 2), n * HID, HID)

    def compute2(b, t):
        for n in range(t * half // OUT, (t + 1) * half // OUT):
            down(lax.rem(b, slots), n, OUT)
        pack(b, t)

    def next_rows(b):
        @pl.when(b + 2 < blocks)
        def _():
            x_copy(b + 2).start()

    def far(b, t):
        return [(s1s.at[t, b, pl.ds(w * h, h)], s1r.at[t, w, b], first[t][w]) for w in range(2)]

    def near(b, t, own_half):
        k = [pl.ds((1 - w if own_half else w) * h, h) for w in range(2)]
        return [(s2s.at[t, w, b, k[w]], s2r.at[t, w, b, k[w]], first[t][w]) for w in range(2)]

    def far2(lo, n, t):
        bs = pl.ds(lo, n)
        return [(s3s.at[t, bs, :, pl.ds(w * quarter, quarter)], s3r.at[t, w, bs], second[t][w])
                for w in range(2)]

    def near2(lo, n, t):
        bs = pl.ds(lo, n)
        return [(s4s.at[t, w, bs], s4r.at[t, w, bs], second[t][w]) for w in range(2)]

    def gather1(lo, n, t):
        p, q = pos[t]
        at = y.at[pl.ds(lo, n), ds(p * sec + q * piece, piece), pl.ds(t * half, half)]
        return [(at, at, second[t][w]) for w in range(2)]

    def gather2(lo, n, t):
        p, q = pos[t]
        at = [y.at[pl.ds(lo, n), ds(p * sec + v * piece, piece),
                   pl.ds(t * half + w * quarter, quarter)] for w, v in enumerate((dn1(q), up1(q)))]
        return [(at[w], at[w], second[t][w]) for w in range(2)]

    def gather3(lo, n, t):
        p, _ = pos[t]
        at = y.at[pl.ds(lo, n), ds(p * sec, sec), pl.ds(t * half, half)]
        return [(at, at, first[t][w]) for w in range(2)]

    def gather4(lo, n, t):
        p, _ = pos[t]
        at = [y.at[pl.ds(lo, n), ds(v * sec + w * h, h), pl.ds(t * half, half)]
              for w, v in enumerate((dn1(p), up1(p)))]
        return [(at[w], at[w], first[t][w]) for w in range(2)]

    FAR, NEAR = 0, blocks
    S_FAR, S_NEAR, S_FAR2, S_NEAR2 = range(4)

    def start(copies, sent, sem):
        for src, dst, to in copies:
            pltpu.make_async_remote_copy(
                src_ref=src, dst_ref=dst, send_sem=send_sem.at[sent], recv_sem=recv_sem.at[sem],
                device_id={"tp": to}, device_id_type=MESH).start()

    def arrive(like, sem):
        pltpu.make_async_copy(like, like, recv_sem.at[sem]).wait()

    def pack(b, t):
        slot = lax.rem(b, slots)
        p, _ = pos[t]
        c = pl.ds(t * half, half)
        s1s[t, b] = term[slot, ds(opp(p) * sec, sec), c].astype(bf16)
        start(far(b, t), S_FAR, FAR + b)
        s2s[t, 0, b, pl.ds(h, h)] = term[slot, ds(up1(p) * sec + h, h), c].astype(bf16)
        s2s[t, 1, b, pl.ds(0, h)] = term[slot, ds(dn1(p) * sec, h), c].astype(bf16)
        start(near(b, t, True), S_NEAR, NEAR + b)

    def reduce1(b):
        slot = lax.rem(b, slots)
        arrive(s1r.at[:, :, b], FAR + b)
        for t in range(2):
            p, _ = pos[t]
            c = pl.ds(t * half, half)
            s2s[t, 0, b, pl.ds(0, h)] = (
                term[slot, ds(up1(p) * sec, h), c] + s1r[t, 0, b].astype(f32)).astype(bf16)
            s2s[t, 1, b, pl.ds(h, h)] = (
                term[slot, ds(dn1(p) * sec + h, h), c] + s1r[t, 1, b].astype(f32)).astype(bf16)
            start(near(b, t, False), S_NEAR, NEAR + b)
        for t in range(2):
            p, _ = pos[t]
            own[t, b] = term[slot, ds(p * sec, sec), pl.ds(t * half, half)]

    def reduce2(lo, n):
        for b in range(lo, lo + n):
            arrive(s2r.at[:, :, b], NEAR + b)
        for t in range(2):
            _, q = pos[t]
            for b in range(lo, lo + n):
                own[t, b] = own[t, b] + s2r[t, 0, b].astype(f32) + s2r[t, 1, b].astype(f32)
                s3s[t, b] = own[t, b, ds(opp(q) * piece, piece), :].astype(bf16)
            start(far2(lo, n, t), S_FAR2, FAR + lo + 1)

    def reduce3(lo, n):
        left, right = pl.ds(0, quarter), pl.ds(quarter, quarter)
        arrive(s3r.at[:, :, pl.ds(lo, n)], FAR + lo + 1)
        for t in range(2):
            _, q = pos[t]
            r, l = ds(up1(q) * piece, piece), ds(dn1(q) * piece, piece)
            for b in range(lo, lo + n):
                s4s[t, 0, b, :, left] = (
                    own[t, b, r, left] + s3r[t, 0, b].astype(f32)).astype(bf16)
                s4s[t, 0, b, :, right] = own[t, b, r, right].astype(bf16)
                s4s[t, 1, b, :, left] = own[t, b, l, left].astype(bf16)
                s4s[t, 1, b, :, right] = (
                    own[t, b, l, right] + s3r[t, 1, b].astype(f32)).astype(bf16)
            start(near2(lo, n, t), S_NEAR2, NEAR + lo + 1)

    def reduce4(lo, n):
        arrive(s4r.at[:, :, pl.ds(lo, n)], NEAR + lo + 1)
        for t in range(2):
            p, q = pos[t]
            for b in range(lo, lo + n):
                y[b, ds(p * sec + q * piece, piece), pl.ds(t * half, half)] = (
                    own[t, b, ds(q * piece, piece), :]
                    + s4r[t, 0, b].astype(f32) + s4r[t, 1, b].astype(f32)).astype(bf16)
            start(gather1(lo, n, t), S_NEAR2, FAR + lo + 1)

    def send2(lo, n):
        arrive(s4r.at[:, :, pl.ds(lo, n)], FAR + lo + 1)
        for t in range(2):
            start(gather2(lo, n, t), S_FAR2, NEAR + lo + 1)

    def got2(lo, n):
        arrive(s3r.at[:, :, pl.ds(lo, n)], NEAR + lo + 1)

    def send3(lo, n):
        for t in range(2):
            start(gather3(lo, n, t), S_NEAR, FAR + lo)

    def send4(lo, n):
        arrive(s2r.at[:, :, pl.ds(lo, n)], FAR + lo)
        for t in range(2):
            start(gather4(lo, n, t), S_FAR, NEAR + lo)

    def got4(lo, n):
        arrive(s1r.at[:, :, pl.ds(lo, n)], NEAR + lo)

    x_copy(0).wait()
    for n in range(3):
        for c in load_in(n):
            c.wait()
        if n == 0:
            for k in range(d // OUT0):
                load_out(k).start()
            x_copy(1).start()
        hidden(0, *pieces0[n])
    for t in range(2):
        for n in range(t * half // OUT0, (t + 1) * half // OUT0):
            load_out(n).wait()
            down(0, n, OUT0)
        if t == 0:
            pl.semaphore_wait(barrier, 4)
        pack(0, t)
    x_copy(2).start()

    compute1(1)
    compute2(1, 0)
    reduce1(0)
    compute2(1, 1)
    next_rows(1)

    pair = [(b, 2) for b in range(0, blocks, 2)]
    beside = {
        5: [(reduce2, *pair[0])],
        6: [(reduce2, *pair[1]), (reduce3, *pair[0])],
        7: [(reduce3, *pair[1]), (reduce4, *pair[0])],
    }

    def step(b, _):
        compute1(b)
        compute2(b, 0)
        compute2(b, 1)
        next_rows(b)
        reduce1(b - 1)

        for k, tasks in beside.items():
            @pl.when(b == k)
            def _():
                for task, *args in tasks:
                    task(*args)
        return 0

    lax.fori_loop(2, blocks, step, 0)

    for task, *args in [
        (reduce1, blocks - 1),
        (reduce2, *pair[2]), (reduce4, *pair[1]), (send2, *pair[0]),
        (reduce3, *pair[2]), (reduce2, *pair[3]), (send2, *pair[1]),
        (got2, *pair[0]), (send3, 0, 2),
        (reduce4, *pair[2]), (reduce3, *pair[3]),
        (got2, *pair[1]), (send3, 2, 2),
        (send2, *pair[2]), (reduce4, *pair[3]),
        (got2, *pair[2]), (send3, 4, 2),
        (send2, *pair[3]), (send4, 0, 2),
        (got2, *pair[3]), (send3, 6, 1), (send3, 7, 1),
        (send4, 2, 2), (send4, 4, 2), (send4, 6, 1), (send4, 7, 1),
        (got4, 0, 2), (got4, 2, 2), (got4, 4, 2), (got4, 6, 1), (got4, 7, 1),
    ]:
        task(*args)

    for sent, like in enumerate((s2s, y, s4s, s1s)):
        pltpu.make_async_copy(like, like, send_sem.at[sent]).wait()


def solution(mesh):
    side = math.isqrt(mesh.shape["tp"])

    def step(x, w_gate, w_up, w_down):
        rows, d = x.shape
        f = w_gate.shape[1]
        blocks, sec = rows // BLOCK, BLOCK // side
        piece, half = sec // side, d // 2
        bf16, f32 = jnp.bfloat16, jnp.float32
        return pl.pallas_call(
            functools.partial(kernel, side),
            out_shape=pltpu.VMEM((blocks, BLOCK, d), bf16),
            in_specs=[pl.BlockSpec(memory_space=pl.ANY)] * 4,
            out_specs=pl.BlockSpec(memory_space=pltpu.VMEM),
            scratch_shapes=[
                pltpu.VMEM((2, BLOCK, d), bf16),
                pltpu.VMEM((d, f), bf16),
                pltpu.VMEM((d, f), bf16),
                pltpu.VMEM((f, d), bf16),
                pltpu.VMEM((BLOCK, f), bf16),
                pltpu.VMEM((4, BLOCK, d), f32),
                pltpu.VMEM((2, blocks, sec, half), f32),
                pltpu.VMEM((2, blocks, sec, half), bf16),
                pltpu.VMEM((2, 2, blocks, sec // 2, half), bf16),
                pltpu.VMEM((2, 2, blocks, sec, half), bf16),
                pltpu.VMEM((2, 2, blocks, sec, half), bf16),
                pltpu.VMEM((2, blocks, piece, half), bf16),
                pltpu.VMEM((2, 2, blocks, piece, half // 2), bf16),
                pltpu.VMEM((2, 2, blocks, piece, half), bf16),
                pltpu.VMEM((2, 2, blocks, piece, half), bf16),
                pltpu.SemaphoreType.DMA((2,)),
                pltpu.SemaphoreType.DMA((3,)),
                pltpu.SemaphoreType.DMA((3,)),
                pltpu.SemaphoreType.DMA((d // OUT0,)),
                pltpu.SemaphoreType.DMA((4,)),
                pltpu.SemaphoreType.DMA((2 * blocks,)),
            ],
            compiler_params=pltpu.CompilerParams(
                collective_id=0, has_side_effects=True, vmem_limit_bytes=50 * 2**20),
        )(x, w_gate, w_up, w_down).reshape(rows, d)

    return jax.shard_map(
        step,
        mesh=mesh,
        in_specs=(P("dp", None), P(None, "tp"), P(None, "tp"), P("tp", None)),
        out_specs=P("dp", None),
        check_vma=False,
    )
```

```python
import functools
import math

import jax
import jax.numpy as jnp
from jax import lax
from jax.experimental import pallas as pl
from jax.experimental.pallas import tpu as pltpu
from jax.sharding import PartitionSpec as P

MESH = pl.DeviceIdType.MESH
BLOCK = 256
HID0, OUT0 = 256, 1024
HID, OUT = 1024, 1024


def kernel(side, x_hbm, wg_hbm, wu_hbm, wd_hbm, y, xb, wg, wu, wd, hid, term, own,
           s1s, s1r, s2s, s2r, s3s, s3r, s4s, s4r, x_sem, wg_sem, wu_sem, wd_sem,
           send_sem, recv_sem):
    rows, d = x_hbm.shape
    f = wg.shape[1]
    blocks = rows // BLOCK
    sec = BLOCK // side
    piece = sec // side
    h = sec // 2
    half = d // 2
    quarter = half // 2
    slots = term.shape[0]
    f32, bf16 = jnp.float32, jnp.bfloat16

    me = lax.axis_index("tp")
    i, j = me // side, me % side

    def up1(v):
        return lax.rem(v + 1, side)

    def dn1(v):
        return lax.rem(v + side - 1, side)

    def opp(v):
        return lax.rem(v + 2, side)

    along_x = (up1(i) * side + j, dn1(i) * side + j)
    along_y = (i * side + up1(j), i * side + dn1(j))
    first = (along_x, along_y)
    second = (along_y, along_x)
    pos = ((i, j), (j, i))

    barrier = pltpu.get_barrier_semaphore()
    for n in along_x + along_y:
        pl.semaphore_signal(barrier, inc=1, device_id={"tp": n}, device_id_type=MESH)

    def ds(start, size):
        return pl.ds(pl.multiple_of(start, size), size)

    def x_copy(b):
        return pltpu.make_async_copy(
            x_hbm.at[ds(b * BLOCK, BLOCK)], xb.at[lax.rem(b, 2)], x_sem.at[lax.rem(b, 2)])

    pieces0 = [(0, HID0), (HID0, HID0), (2 * HID0, f - 2 * HID0)]

    def load(src, dst, sem, n, first_col, size):
        cols = pl.ds(first_col, size)
        return pltpu.make_async_copy(src.at[:, cols], dst.at[:, cols], sem.at[n])

    def load_in(n):
        return load(wg_hbm, wg, wg_sem, n, *pieces0[n]), load(wu_hbm, wu, wu_sem, n, *pieces0[n])

    def load_out(n):
        return load(wd_hbm, wd, wd_sem, n, n * OUT0, OUT0)

    x_copy(0).start()
    for n in range(3):
        for c in load_in(n):
            c.start()

    def hidden(xs, first_col, size):
        cols = pl.ds(first_col, size)
        gate = jnp.dot(xb[xs], wg[:, cols], preferred_element_type=f32)
        up = jnp.dot(xb[xs], wu[:, cols], preferred_element_type=f32)
        hid[:, cols] = (jax.nn.gelu(gate) * up).astype(bf16)

    def down(slot, n, size):
        cols = pl.ds(n * size, size)
        term[slot, :, cols] = jnp.dot(hid[...], wd[:, cols], preferred_element_type=f32)

    def compute1(b):
        x_copy(b).wait()
        for n in range(f // HID):
            hidden(lax.rem(b, 2), n * HID, HID)

    def compute2(b, t):
        for n in range(t * half // OUT, (t + 1) * half // OUT):
            down(lax.rem(b, slots), n, OUT)
        pack(b, t)

    def next_rows(b):
        @pl.when(b + 2 < blocks)
        def _():
            x_copy(b + 2).start()

    def far(b, t):
        return [(s1s.at[t, b, pl.ds(w * h, h)], s1r.at[t, w, b], first[t][w]) for w in range(2)]

    def near(b, t, own_half):
        k = [pl.ds((1 - w if own_half else w) * h, h) for w in range(2)]
        return [(s2s.at[t, w, b, k[w]], s2r.at[t, w, b, k[w]], first[t][w]) for w in range(2)]

    def far2(lo, n, t):
        bs = pl.ds(lo, n)
        return [(s3s.at[t, bs, :, pl.ds(w * quarter, quarter)], s3r.at[t, w, bs], second[t][w])
                for w in range(2)]

    def near2(lo, n, t):
        bs = pl.ds(lo, n)
        return [(s4s.at[t, w, bs], s4r.at[t, w, bs], second[t][w]) for w in range(2)]

    def gather1(lo, n, t):
        p, q = pos[t]
        at = y.at[pl.ds(lo, n), ds(p * sec + q * piece, piece), pl.ds(t * half, half)]
        return [(at, at, second[t][w]) for w in range(2)]

    def gather2(lo, n, t):
        p, q = pos[t]
        at = [y.at[pl.ds(lo, n), ds(p * sec + v * piece, piece),
                   pl.ds(t * half + w * quarter, quarter)] for w, v in enumerate((dn1(q), up1(q)))]
        return [(at[w], at[w], second[t][w]) for w in range(2)]

    def gather3(lo, n, t):
        p, _ = pos[t]
        at = y.at[pl.ds(lo, n), ds(p * sec, sec), pl.ds(t * half, half)]
        return [(at, at, first[t][w]) for w in range(2)]

    def gather4(lo, n, t):
        p, _ = pos[t]
        at = [y.at[pl.ds(lo, n), ds(v * sec + w * h, h), pl.ds(t * half, half)]
              for w, v in enumerate((dn1(p), up1(p)))]
        return [(at[w], at[w], first[t][w]) for w in range(2)]

    FAR, NEAR, AHEAD = 0, blocks, 2 * blocks
    S_FAR, S_NEAR, S_FAR2, S_NEAR2 = range(4)

    def start(copies, sent, sem):
        for src, dst, to in copies:
            pltpu.make_async_remote_copy(
                src_ref=src, dst_ref=dst, send_sem=send_sem.at[sent], recv_sem=recv_sem.at[sem],
                device_id={"tp": to}, device_id_type=MESH).start()

    def arrive(like, sem):
        pltpu.make_async_copy(like, like, recv_sem.at[sem]).wait()

    def pack(b, t):
        slot = lax.rem(b, slots)
        p, _ = pos[t]
        c = pl.ds(t * half, half)
        s1s[t, b] = term[slot, ds(opp(p) * sec, sec), c].astype(bf16)
        start(far(b, t), S_FAR, (FAR, AHEAD)[t] + b)
        s2s[t, 0, b, pl.ds(h, h)] = term[slot, ds(up1(p) * sec + h, h), c].astype(bf16)
        s2s[t, 1, b, pl.ds(0, h)] = term[slot, ds(dn1(p) * sec, h), c].astype(bf16)
        start(near(b, t, True), S_NEAR, NEAR + b)

    def reduce1(b):
        slot = lax.rem(b, slots)
        for t in range(2):
            arrive(s1r.at[t, :, b], (FAR, AHEAD)[t] + b)
            p, _ = pos[t]
            c = pl.ds(t * half, half)
            s2s[t, 0, b, pl.ds(0, h)] = (
                term[slot, ds(up1(p) * sec, h), c] + s1r[t, 0, b].astype(f32)).astype(bf16)
            s2s[t, 1, b, pl.ds(h, h)] = (
                term[slot, ds(dn1(p) * sec + h, h), c] + s1r[t, 1, b].astype(f32)).astype(bf16)
            start(near(b, t, False), S_NEAR, NEAR + b)
        for t in range(2):
            p, _ = pos[t]
            own[t, b] = term[slot, ds(p * sec, sec), pl.ds(t * half, half)]

    def reduce2(lo, n):
        for b in range(lo, lo + n):
            arrive(s2r.at[:, :, b], NEAR + b)
        for t in range(2):
            _, q = pos[t]
            for b in range(lo, lo + n):
                own[t, b] = own[t, b] + s2r[t, 0, b].astype(f32) + s2r[t, 1, b].astype(f32)
                s3s[t, b] = own[t, b, ds(opp(q) * piece, piece), :].astype(bf16)
            start(far2(lo, n, t), S_FAR2, FAR + lo + 1)

    def reduce3(lo, n):
        left, right = pl.ds(0, quarter), pl.ds(quarter, quarter)
        arrive(s3r.at[:, :, pl.ds(lo, n)], FAR + lo + 1)
        for t in range(2):
            _, q = pos[t]
            r, l = ds(up1(q) * piece, piece), ds(dn1(q) * piece, piece)
            for b in range(lo, lo + n):
                s4s[t, 0, b, :, left] = (
                    own[t, b, r, left] + s3r[t, 0, b].astype(f32)).astype(bf16)
                s4s[t, 0, b, :, right] = own[t, b, r, right].astype(bf16)
                s4s[t, 1, b, :, left] = own[t, b, l, left].astype(bf16)
                s4s[t, 1, b, :, right] = (
                    own[t, b, l, right] + s3r[t, 1, b].astype(f32)).astype(bf16)
            start(near2(lo, n, t), S_NEAR2, NEAR + lo + 1)

    def reduce4(lo, n):
        arrive(s4r.at[:, :, pl.ds(lo, n)], NEAR + lo + 1)
        for t in range(2):
            p, q = pos[t]
            for b in range(lo, lo + n):
                y[b, ds(p * sec + q * piece, piece), pl.ds(t * half, half)] = (
                    own[t, b, ds(q * piece, piece), :]
                    + s4r[t, 0, b].astype(f32) + s4r[t, 1, b].astype(f32)).astype(bf16)
            start(gather1(lo, n, t), S_NEAR2, FAR + lo + 1)

    def send2(lo, n):
        arrive(s4r.at[:, :, pl.ds(lo, n)], FAR + lo + 1)
        for t in range(2):
            start(gather2(lo, n, t), S_FAR2, NEAR + lo + 1)

    def got2(lo, n):
        arrive(s3r.at[:, :, pl.ds(lo, n)], NEAR + lo + 1)

    def send3(lo, n):
        for t in range(2):
            start(gather3(lo, n, t), S_NEAR, FAR + lo)

    def send4(lo, n):
        arrive(s2r.at[:, :, pl.ds(lo, n)], FAR + lo)
        for t in range(2):
            start(gather4(lo, n, t), S_FAR, NEAR + lo)

    def got4(lo, n):
        arrive(s1r.at[:, :, pl.ds(lo, n)], NEAR + lo)

    x_copy(0).wait()
    for n in range(3):
        for c in load_in(n):
            c.wait()
        if n == 0:
            for k in range(d // OUT0):
                load_out(k).start()
            x_copy(1).start()
        hidden(0, *pieces0[n])
    for t in range(2):
        for n in range(t * half // OUT0, (t + 1) * half // OUT0):
            load_out(n).wait()
            down(0, n, OUT0)
        if t == 0:
            pl.semaphore_wait(barrier, 4)
        pack(0, t)
    x_copy(2).start()

    compute1(1)
    compute2(1, 0)
    reduce1(0)
    compute2(1, 1)
    next_rows(1)

    pair = [(b, 2) for b in range(0, blocks, 2)]
    beside = {
        5: [(reduce2, *pair[0])],
        6: [(reduce2, *pair[1]), (reduce3, *pair[0])],
        7: [(reduce3, *pair[1]), (reduce4, *pair[0])],
    }

    def step(b, _):
        compute1(b)
        compute2(b, 0)
        compute2(b, 1)
        next_rows(b)
        reduce1(b - 1)

        for k, tasks in beside.items():
            @pl.when(b == k)
            def _():
                for task, *args in tasks:
                    task(*args)
        return 0

    lax.fori_loop(2, blocks, step, 0)

    for task, *args in [
        (reduce1, blocks - 1),
        (reduce2, *pair[2]), (reduce4, *pair[1]), (send2, *pair[0]),
        (reduce3, *pair[2]), (reduce2, *pair[3]), (send2, *pair[1]),
        (got2, *pair[0]), (send3, 0, 2),
        (reduce4, *pair[2]), (reduce3, *pair[3]),
        (got2, *pair[1]), (send3, 2, 2),
        (send2, *pair[2]), (reduce4, *pair[3]),
        (got2, *pair[2]), (send3, 4, 2),
        (send2, *pair[3]), (send4, 0, 2),
        (got2, *pair[3]), (send3, 6, 1), (send3, 7, 1),
        (send4, 2, 2), (send4, 4, 2), (send4, 6, 1), (send4, 7, 1),
        (got4, 0, 2), (got4, 2, 2), (got4, 4, 2), (got4, 6, 1), (got4, 7, 1),
    ]:
        task(*args)

    for sent, like in enumerate((s2s, y, s4s, s1s)):
        pltpu.make_async_copy(like, like, send_sem.at[sent]).wait()


def solution(mesh):
    side = math.isqrt(mesh.shape["tp"])

    def step(x, w_gate, w_up, w_down):
        rows, d = x.shape
        f = w_gate.shape[1]
        blocks, sec = rows // BLOCK, BLOCK // side
        piece, half = sec // side, d // 2
        bf16, f32 = jnp.bfloat16, jnp.float32
        return pl.pallas_call(
            functools.partial(kernel, side),
            out_shape=pltpu.VMEM((blocks, BLOCK, d), bf16),
            in_specs=[pl.BlockSpec(memory_space=pl.ANY)] * 4,
            out_specs=pl.BlockSpec(memory_space=pltpu.VMEM),
            scratch_shapes=[
                pltpu.VMEM((2, BLOCK, d), bf16),
                pltpu.VMEM((d, f), bf16),
                pltpu.VMEM((d, f), bf16),
                pltpu.VMEM((f, d), bf16),
                pltpu.VMEM((BLOCK, f), bf16),
                pltpu.VMEM((4, BLOCK, d), f32),
                pltpu.VMEM((2, blocks, sec, half), f32),
                pltpu.VMEM((2, blocks, sec, half), bf16),
                pltpu.VMEM((2, 2, blocks, sec // 2, half), bf16),
                pltpu.VMEM((2, 2, blocks, sec, half), bf16),
                pltpu.VMEM((2, 2, blocks, sec, half), bf16),
                pltpu.VMEM((2, blocks, piece, half), bf16),
                pltpu.VMEM((2, 2, blocks, piece, half // 2), bf16),
                pltpu.VMEM((2, 2, blocks, piece, half), bf16),
                pltpu.VMEM((2, 2, blocks, piece, half), bf16),
                pltpu.SemaphoreType.DMA((2,)),
                pltpu.SemaphoreType.DMA((3,)),
                pltpu.SemaphoreType.DMA((3,)),
                pltpu.SemaphoreType.DMA((d // OUT0,)),
                pltpu.SemaphoreType.DMA((4,)),
                pltpu.SemaphoreType.DMA((3 * blocks,)),
            ],
            compiler_params=pltpu.CompilerParams(
                collective_id=0, has_side_effects=True, vmem_limit_bytes=50 * 2**20),
        )(x, w_gate, w_up, w_down).reshape(rows, d)

    return jax.shard_map(
        step,
        mesh=mesh,
        in_specs=(P("dp", None), P(None, "tp"), P(None, "tp"), P("tp", None)),
        out_specs=P("dp", None),
        check_vma=False,
    )
```
